256 devices in a mesh: gx: 4 (over z_lo), gy: 8 (over z_hi, x), gz: 8 (over y, core).
Axes of the slice: x: 4, y: 4, z: 8 (z_hi: 2, z_lo: 4; z = z_hi * 4 + z_lo), core: 2. Of those that a mesh axis runs over, the one named last changes fastest.
Arguments:
- volume: bfloat16 [32, 8, 128, 1024], P(None, 'gx', 'gy', 'gz'), may hold values from -6 to 6
- w_first: bfloat16 [3, 3, 3, 32, 32], replicated, may hold values from -0.21875 to 0.21875
- w_second: bfloat16 [3, 3, 3, 32, 32], replicated, may hold values from -0.21875 to 0.21875
- v_first: bfloat16 [3, 3, 3, 32, 32], replicated, may hold values from -0.21875 to 0.21875
- v_second: bfloat16 [3, 3, 3, 32, 32], replicated, may hold values from -0.21875 to 0.21875
Outputs:
- jv: bfloat16 [32, 8, 128, 1024], P(None, 'gx', 'gy', 'gz')
- gv_first: float32 [3, 3, 3, 32, 32], replicated
- gv_second: float32 [3, 3, 3, 32, 32], replicated
The draws below stay inside these ranges and needn't reach their ends.
All inputs are finite; a program needn't handle non-finite values.
Results may differ from the reference program's by a relative error of at most 0.005.
Values may be sent and summed in bfloat16 or wider, within the bound.
A program may use at most 64 MiB of HBM per device.

```python
import jax
import jax.numpy as jnp
from jax import lax

CHANNELS = 32
NX = 8
NY = 128
NZ = 1024
CELLS = 1048576
FILT = 864


def shard_levels(key, extent, split, least, high):
    factor_of, own = 1.0, jax.random.fold_in(key, 6)
    for dim, parts in split:
        heights = jnp.exp(jax.random.uniform(jax.random.fold_in(own, dim), (parts,), jnp.float32, least / len(split), high / len(split)))
        factor_of = factor_of * jnp.repeat(heights, extent[dim] // parts).reshape([-1 if axis == dim else 1 for axis in range(len(extent))])
    return factor_of


def bell_draw(key, dims, deviation, bound, shards=(), held_as=jnp.bfloat16):
    gain = shard_levels(key, dims, shards, -0.22, 0.18) if shards else 1.0
    drawn = jax.random.normal(key, dims, jnp.float32) * deviation * gain
    return jnp.minimum(jnp.maximum(drawn, -bound), bound).astype(held_as)


def setup_inputs(seed: int = 0) -> dict:
    key_of = jax.random.split(jax.random.key(seed), 6)
    return {
        "volume": bell_draw(key_of[0], (CHANNELS, NX, NY, NZ), 1.0, 6.0, ((1, 4), (2, 8), (3, 8))),
        "w_first": bell_draw(key_of[1], (3, 3, 3, CHANNELS, CHANNELS), FILT ** -0.5, 0.21875),
        "w_second": bell_draw(key_of[2], (3, 3, 3, CHANNELS, CHANNELS), FILT ** -0.5, 0.21875),
        "v_first": bell_draw(key_of[3], (3, 3, 3, CHANNELS, CHANNELS), FILT ** -0.5, 0.21875),
        "v_second": bell_draw(key_of[4], (3, 3, 3, CHANNELS, CHANNELS), FILT ** -0.5, 0.21875),
    }


def gelu_pair(pre):
    inner = 0.7978845608 * (pre + 0.044715 * pre * pre * pre)
    hyper = jnp.tanh(inner)
    hidden = 0.5 * pre * (1.0 + hyper)
    slope = 0.5 * (1.0 + hyper) + 0.5 * pre * (1.0 - hyper * hyper) * 0.7978845608 * (1.0 + 0.134145 * pre * pre)
    return hidden, slope


def convolve(field, weight):
    result = lax.conv_general_dilated(field.astype(jnp.float32)[None], weight.astype(jnp.float32), (1, 1, 1), "SAME", dimension_numbers=("NCDHW", "DHWIO", "NCDHW"), precision=lax.Precision.HIGHEST)
    return result[0]


def correlate(field, target):
    padded = jnp.pad(field.astype(jnp.float32), ((0, 0), (1, 1), (1, 1), (1, 1)))
    target32 = target.astype(jnp.float32)
    sizes = field.shape
    planes = []
    for shift_x in range(3):
        rows_y = []
        for shift_y in range(3):
            rows_z = []
            for shift_z in range(3):
                window = padded[:, shift_x:shift_x + sizes[1], shift_y:shift_y + sizes[2], shift_z:shift_z + sizes[3]]
                rows_z.append(jnp.einsum("cxyz,oxyz->co", window, target32, precision=lax.Precision.HIGHEST))
            rows_y.append(jnp.stack(rows_z))
        planes.append(jnp.stack(rows_y))
    return jnp.stack(planes)


def reference(volume, w_first, w_second, v_first, v_second):
    pre = convolve(volume, w_first)
    hidden_f, slope = gelu_pair(pre)
    hidden = hidden_f.astype(jnp.bfloat16)
    tangent = (slope * convolve(volume, v_first)).astype(jnp.bfloat16)
    jv = (convolve(tangent, w_second) + convolve(hidden, v_second)).astype(jnp.bfloat16)
    flipped = jnp.transpose(jnp.flip(w_second, (0, 1, 2)), (0, 1, 2, 4, 3))
    back = (slope * convolve(jv, flipped)).astype(jnp.bfloat16)
    count_all = jnp.float32(CELLS)
    factor = jnp.float32(FILT) ** 0.5
    gv_second = factor * (correlate(hidden, jv) / count_all + 0.1 * v_second.astype(jnp.float32))
    gv_first = factor * (correlate(volume, back) / count_all + 0.1 * v_first.astype(jnp.float32))
    return jv, gv_first, gv_second
```

```python
import functools
import math

import jax
import jax.numpy as jnp
from jax import lax
from jax.experimental import pallas as pl
from jax.experimental.pallas import tpu as pltpu
from jax.sharding import PartitionSpec as P

MESH = pl.DeviceIdType.MESH


def reduce_kernel(nx, ny, nz, x_ref, o_ref, recv1, rows, recv2, gath, chunk, s1, r1, s2, r2, s3, r3, s4, r4):
    ix, iy, iz = lax.axis_index("gx"), lax.axis_index("gy"), lax.axis_index("gz")
    plane = nx * ny
    me = iy * nx + ix

    def z_peer(d):
        return {"gx": ix, "gy": iy, "gz": lax.rem(iz + d, nz)}

    def p_peer(d):
        q = lax.rem(me + d, plane)
        return q, {"gx": lax.rem(q, nx), "gy": q // nx, "gz": iz}

    barrier = pltpu.get_barrier_semaphore()
    for d in range(1, nz):
        pl.semaphore_signal(barrier, inc=1, device_id=z_peer(d), device_id_type=MESH)

    def greet(d, _):
        pl.semaphore_signal(barrier, inc=1, device_id=p_peer(d)[1], device_id_type=MESH)
        return 0

    lax.fori_loop(1, plane, greet, 0)
    pl.semaphore_wait(barrier, nz - 1 + plane - 1)

    def send1(d):
        peer = z_peer(d)
        return pltpu.make_async_remote_copy(
            x_ref.at[peer["gz"]], recv1.at[d - 1], s1.at[d - 1], r1.at[d - 1], device_id=peer, device_id_type=MESH
        )

    for d in range(1, nz):
        send1(d).start()
    total = x_ref[iz]
    for d in range(1, nz):
        send1(d).wait_recv()
        total = total + recv1[d - 1]
    for f in range(2):
        for q in range(plane):
            rows[q, f : f + 1, :] = total[f, q // 8, q % 8 : q % 8 + 1, :]

    def send2(d):
        q, peer = p_peer(d)
        return pltpu.make_async_remote_copy(
            rows.at[q], recv2.at[d - 1], s2.at[d - 1], r2.at[d - 1], device_id=peer, device_id_type=MESH
        )

    def send3(d):
        q, peer = p_peer(d)
        return pltpu.make_async_remote_copy(
            gath.at[me], gath.at[me], s3.at[d - 1], r3.at[d - 1], device_id=peer, device_id_type=MESH
        )

    def start2(d, _):
        send2(d).start()
        return 0

    def take2(d, acc):
        send2(d).wait_recv()
        return acc + recv2[d - 1]

    def start3(d, _):
        send3(d).start()
        return 0

    def take3(d, _):
        send3(d).wait_recv()
        return 0

    lax.fori_loop(1, plane, start2, 0)
    gath[me] = lax.fori_loop(1, plane, take2, rows[me])
    lax.fori_loop(1, plane, start3, 0)
    lax.fori_loop(1, plane, take3, 0)
    for f in range(2):
        for q in range(plane):
            chunk[f, q // 8, q % 8 : q % 8 + 1, :] = gath[q, f : f + 1, :]

    def send4(d):
        return pltpu.make_async_remote_copy(
            chunk, o_ref.at[iz], s4.at[d - 1], r4.at[d - 1], device_id=z_peer(d), device_id_type=MESH
        )

    for d in range(1, nz):
        send4(d).start()
    o_ref[iz] = chunk[...]
    for d in range(1, nz):
        send4(d).wait_recv()
    for d in range(1, nz):
        send1(d).wait_send()
        send4(d).wait_send()

    def drain(d, _):
        send2(d).wait_send()
        send3(d).wait_send()
        return 0

    lax.fori_loop(1, plane, drain, 0)


def all_sums(first, second):
    nx, ny, nz = lax.axis_size("gx"), lax.axis_size("gy"), lax.axis_size("gz")
    plane = nx * ny
    tiles = plane // 8
    size = first.size
    whole = nz * plane * 128
    flat = jnp.stack([first.reshape(-1), second.reshape(-1)])
    flat = jnp.pad(flat, ((0, 0), (0, whole - size))).reshape(2, nz, tiles, 8, 128)
    flat = jnp.transpose(flat, (1, 0, 2, 3, 4))
    dma = pltpu.SemaphoreType.DMA
    out = pl.pallas_call(
        functools.partial(reduce_kernel, nx, ny, nz),
        out_shape=jax.ShapeDtypeStruct((nz, 2, tiles, 8, 128), jnp.float32),
        in_specs=[pl.BlockSpec(memory_space=pltpu.VMEM)],
        out_specs=pl.BlockSpec(memory_space=pltpu.VMEM),
        scratch_shapes=[
            pltpu.VMEM((nz - 1, 2, tiles, 8, 128), jnp.float32),
            pltpu.VMEM((plane, 2, 128), jnp.float32),
            pltpu.VMEM((plane - 1, 2, 128), jnp.float32),
            pltpu.VMEM((plane, 2, 128), jnp.float32),
            pltpu.VMEM((2, tiles, 8, 128), jnp.float32),
            dma((nz - 1,)), dma((nz - 1,)),
            dma((plane - 1,)), dma((plane - 1,)),
            dma((plane - 1,)), dma((plane - 1,)),
            dma((nz - 1,)), dma((nz - 1,)),
        ],
        compiler_params=pltpu.CompilerParams(collective_id=0, has_side_effects=True),
    )(flat)
    out = jnp.transpose(out, (1, 0, 2, 3, 4)).reshape(2, whole)[:, :size]
    return out[0].reshape(first.shape), out[1].reshape(second.shape)


def padded_2(cells, sides, width):
    for axis, dim in sides:
        count = lax.axis_size(axis)
        ends = count - 1
        head = lax.slice_in_dim(cells, 0, width, axis=dim)
        tail = lax.slice_in_dim(cells, cells.shape[dim] - width, cells.shape[dim], axis=dim)
        cells = jnp.concatenate(
            [
                lax.ppermute(tail, axis, [(i, (i + 1) % count) for i in range(ends)]),
                cells,
                lax.ppermute(head, axis, [((i + 1) % count, i) for i in range(ends)]),
            ],
            axis=dim,
        )
    return cells


def gelu_pair(pre):
    inner = 0.7978845608 * (pre + 0.044715 * pre * pre * pre)
    hyper = jnp.tanh(inner)
    hidden = 0.5 * pre * (1.0 + hyper)
    slope = 0.5 * (1.0 + hyper) + 0.5 * pre * (1.0 - hyper * hyper) * 0.7978845608 * (
        1.0 + 0.134145 * pre * pre
    )
    return (hidden, slope)


def stencil(padded, weight):
    depth = padded.shape[1] - 2
    height = padded.shape[2] - 2
    width = padded.shape[3] - 2
    in_chan = weight.shape[3]
    out_chan = weight.shape[4]
    summed = jnp.zeros((out_chan, depth, height, width), jnp.float32)
    for shift_x in range(3):
        for shift_y in range(3):
            stacked = jnp.concatenate(
                [
                    padded[
                        :,
                        shift_x : shift_x + depth,
                        shift_y : shift_y + height,
                        shift_z : shift_z + width,
                    ]
                    for shift_z in range(3)
                ],
                axis=0,
            )
            matrix = weight[shift_x, shift_y].reshape(3 * in_chan, out_chan)
            summed = summed + jnp.einsum(
                "kxyz,ko->oxyz", stacked, matrix, preferred_element_type=jnp.float32
            )
    return summed


def correlate(padded, target):
    depth = target.shape[1]
    height = target.shape[2]
    width = target.shape[3]
    in_chan = padded.shape[0]
    out_chan = target.shape[0]
    planes = []
    for shift_x in range(3):
        rows_y = []
        for shift_y in range(3):
            stacked = jnp.concatenate(
                [
                    padded[
                        :,
                        shift_x : shift_x + depth,
                        shift_y : shift_y + height,
                        shift_z : shift_z + width,
                    ]
                    for shift_z in range(3)
                ],
                axis=0,
            )
            product = jnp.einsum(
                "kxyz,oxyz->ko", stacked, target, preferred_element_type=jnp.float32
            )
            rows_y.append(product.reshape(3, in_chan, out_chan))
        planes.append(jnp.stack(rows_y))
    return jnp.stack(planes)


def body(volume, w_first, w_second, v_first, v_second):
    channels = volume.shape[0]
    depth = volume.shape[1]
    height = volume.shape[2]
    width = volume.shape[3]
    count_all = float(
        depth * height * width * lax.axis_size("gx") * lax.axis_size("gy") * lax.axis_size("gz")
    )
    factor = math.sqrt(27.0 * channels)
    input_pad = padded_2(volume, (("gx", 1), ("gy", 2), ("gz", 3)), 1)
    pre = stencil(input_pad, w_first)
    hidden_f, slope = gelu_pair(pre)
    hidden = hidden_f.astype(jnp.bfloat16)
    tangent = (slope * stencil(input_pad, v_first)).astype(jnp.bfloat16)
    paired = padded_2(jnp.stack([hidden, tangent]), (("gx", 2), ("gy", 3), ("gz", 4)), 1)
    hidden_pad = paired[0]
    tangent_pad = paired[1]
    jv = (stencil(tangent_pad, w_second) + stencil(hidden_pad, v_second)).astype(jnp.bfloat16)
    local_second = correlate(hidden_pad, jv)
    jv_pad = padded_2(jv, (("gx", 1), ("gy", 2), ("gz", 3)), 1)
    flipped = jnp.transpose(jnp.flip(w_second, (0, 1, 2)), (0, 1, 2, 4, 3))
    back = (slope * stencil(jv_pad, flipped)).astype(jnp.bfloat16)
    local_first = correlate(input_pad, back)
    summed_first, summed_second = all_sums(local_first, local_second)
    gv_first = factor * (summed_first / count_all + 0.1 * v_first.astype(jnp.float32))
    gv_second = factor * (summed_second / count_all + 0.1 * v_second.astype(jnp.float32))
    return (jv, gv_first, gv_second)


def solution(mesh):
    in_specs = (P(None, "gx", "gy", "gz"), P(), P(), P(), P())
    out_specs = (P(None, "gx", "gy", "gz"), P(), P())
    return jax.shard_map(body, mesh=mesh, in_specs=in_specs, out_specs=out_specs, check_vma=False)
```

```python
import functools
import itertools
import math

import jax
import jax.numpy as jnp
from jax import lax
from jax.experimental import pallas as pl
from jax.experimental.pallas import tpu as pltpu
from jax.sharding import PartitionSpec as P

MESH = pl.DeviceIdType.MESH
BF16 = jnp.bfloat16
F32 = jnp.float32
OFFSETS = [o for o in itertools.product((-1, 0, 1), repeat=3) if o != (0, 0, 0)]
SIDES = [(ox, oz) for ox in (-1, 0, 1) for oz in (-1, 1)]


def gelu_pair(pre):
    square = pre * pre
    hyper = jnp.tanh(0.7978845608 * (pre + 0.044715 * square * pre))
    half = 0.5 * (1.0 + hyper)
    hidden = pre * half
    slope = half + (0.5 * pre) * (1.0 - hyper * hyper) * (0.7978845608 * (1.0 + 0.134145 * square))
    return (hidden, slope)


def main_kernel(
    nx, ny, nz, dx, dy, tiles, share,
    vol, w_first, w_second, v_first, v_second,
    tot, jv_out,
    a1, a2, a3, slope_ref, ej, eb, w1t, w2t, w3t,
    pk1, ed1, pk2, ed2, pk3, ed3,
    part, recv1, rows, recv2, gath, chunk,
    xs1, xr1, xs2, xr2, xs3, xr3, ps3, pr3,
    s1, r1, s2, r2, s3, r3, s4, r4,
):
    ix, iy, iz = lax.axis_index("gx"), lax.axis_index("gy"), lax.axis_index("gz")
    plane = nx * ny
    me = iy * nx + ix
    chan = vol.shape[0]
    hx, hy = dx + 2, dy + 4
    lane = lax.broadcasted_iota(jnp.int32, (chan, 128), 1)

    def there(ox, oy, oz):
        ok = None
        for offset, index, count in ((ox, ix, nx), (oy, iy, ny), (oz, iz, nz)):
            if offset:
                one = index < count - 1 if offset > 0 else index > 0
                ok = one if ok is None else jnp.logical_and(ok, one)
        return ok

    def at(ox, oy, oz):
        return {"gx": ix + ox, "gy": iy + oy, "gz": iz + oz}

    def z_peer(d):
        return {"gx": ix, "gy": iy, "gz": lax.rem(iz + d, nz)}

    def p_peer(d):
        q = lax.rem(me + d, plane)
        return q, {"gx": lax.rem(q, nx), "gy": q // nx, "gz": iz}

    barrier = pltpu.get_barrier_semaphore()
    for o in OFFSETS:
        @pl.when(there(*o))
        def _():
            pl.semaphore_signal(barrier, inc=1, device_id=at(*o), device_id_type=MESH)
    for d in range(1, nz):
        pl.semaphore_signal(barrier, inc=1, device_id=z_peer(d), device_id_type=MESH)

    def greet(d, _):
        pl.semaphore_signal(barrier, inc=1, device_id=p_peer(d)[1], device_id_type=MESH)
        return 0

    lax.fori_loop(1, plane, greet, 0)

    taps = w_first.shape[0]
    w1t[...] = jnp.zeros(w1t.shape, BF16)
    w2t[...] = jnp.zeros(w2t.shape, BF16)
    w3t[...] = jnp.zeros(w3t.shape, BF16)
    w1t[0:chan, 0:taps] = w_first[...].T
    w1t[chan : 2 * chan, 0:taps] = v_first[...].T
    w2t[:, 0:taps] = w_second[...].T
    w2t[:, 896 : 896 + taps] = v_second[...].T
    for k in range(27):
        w3t[:, chan * k : chan * (k + 1)] = w_second[chan * (26 - k) : chan * (27 - k), :]

    def zero(ref):
        ref[...] = jnp.zeros(ref.shape, ref.dtype)

    for x in range(dx):
        a1[dx + x, 3 : 3 + dy, chan : 2 * chan, :] = jnp.transpose(vol[:, x], (1, 0, 2))
        zero(ej.at[x, 0:3])
        zero(ej.at[x, 3 + dy : 5 + dy])
        zero(eb.at[x, 0:3])
        zero(eb.at[x, 3 + dy : 5 + dy])

    def packed(raw, j, pair):
        first = jnp.where(lane == j, jnp.broadcast_to(raw[:, 0:1], raw.shape), pair[0])
        last = jnp.where(lane == j, jnp.broadcast_to(raw[:, 127:128], raw.shape), pair[1])
        return first, last

    blank = jnp.zeros((chan, 128), BF16)

    def pack1(j, pair):
        return packed(a1[dx + j // dy, 3 + lax.rem(j, dy), chan : 2 * chan, :], j, pair)

    pk1[0], pk1[1] = lax.fori_loop(0, dx * dy, pack1, (blank, blank), unroll=4)

    @pl.when(ix == 0)
    def _():
        for x in range(dx):
            zero(a1.at[x, :, chan : 2 * chan, :])
        zero(ed1.at[:, 0])
        zero(a3.at[0])
        zero(ed3.at[:, 0])

    @pl.when(ix == nx - 1)
    def _():
        for x in range(dx):
            zero(a1.at[2 * dx + x, :, chan : 2 * chan, :])
        zero(ed1.at[:, 2])
        zero(a3.at[dx + 1])
        zero(ed3.at[:, 2])

    @pl.when(iy == 0)
    def _():
        for x in range(3 * dx):
            zero(a1.at[x, 0:3, chan : 2 * chan, :])
        zero(ed1.at[:, :, 0])

    @pl.when(iy == ny - 1)
    def _():
        for x in range(3 * dx):
            zero(a1.at[x, 3 + dy : 6 + dy, chan : 2 * chan, :])
        zero(ed1.at[:, :, 2])

    @pl.when(iz == 0)
    def _():
        zero(ed1.at[0])
        zero(ed2.at[0])
        zero(ed3.at[0])

    @pl.when(iz == nz - 1)
    def _():
        zero(ed1.at[1])
        zero(ed2.at[1])
        zero(ed3.at[1])

    def span(index, count):
        return 3 - (index == 0).astype(jnp.int32) - (index == count - 1).astype(jnp.int32)

    near = span(ix, nx) * span(iy, ny) * span(iz, nz) - 1
    pl.semaphore_wait(barrier, near + nz - 1 + plane - 1)

    def send_vol(n):
        ox, oy, oz = OFFSETS[n]
        if oz == 0:
            count = dy if oy == 0 else 3
            src_y = 3 if oy <= 0 else dy
            dst_y = 3 if oy == 0 else (0 if oy > 0 else 3 + dy)
            to_x = dx * (1 - ox)
            src = a1.at[dx : 2 * dx, src_y : src_y + count, chan : 2 * chan, :]
            dst = a1.at[to_x : to_x + dx, dst_y : dst_y + count, chan : 2 * chan, :]
        else:
            src = pk1.at[1 if oz > 0 else 0]
            dst = ed1.at[0 if oz > 0 else 1, 1 - ox, 1 - oy]
        return pltpu.make_async_remote_copy(
            src, dst, xs1.at[n], xr1.at[n], device_id=at(ox, oy, oz), device_id_type=MESH
        )

    for n, o in enumerate(OFFSETS):
        @pl.when(there(*o))
        def _():
            send_vol(n).start()
    for n, o in enumerate(OFFSETS):
        @pl.when(there(*(-c for c in o)))
        def _():
            send_vol(n).wait_recv()

    def shifted(raw, left, right, j):
        before = jnp.where(lane == 0, pltpu.roll(left, lax.rem(128 - j, 128), 1), pltpu.roll(raw, 1, 1))
        after = jnp.where(lane == 127, pltpu.roll(right, 127 - j, 1), pltpu.roll(raw, 127, 1))
        return before, after

    def slab1(i, _):
        x = i // (dy + 6)
        y = lax.rem(i, dy + 6)
        bx = x // dx
        by = (y + dy - 3) // dy
        j = lax.rem(x, dx) * dy + lax.rem(y + dy - 3, dy)
        raw = a1[x, y, chan : 2 * chan, :]
        before, after = shifted(raw, ed1[0, bx, by], ed1[1, bx, by], j)
        a1[x, y, 0:chan, :] = before
        a1[x, y, 2 * chan : 3 * chan, :] = after
        return 0

    lax.fori_loop(0, 3 * dx * (dy + 6), slab1, 0, unroll=4)

    def stacked(ref, x, y):
        halves = []
        for half in range(2):
            pieces = [ref[x + kx, y + half + ky] for kx in range(3) for ky in range(3)]
            pieces.append(ref[x, y + half, 0:chan, :])
            halves.append(jnp.concatenate(pieces, axis=0))
        return jnp.concatenate(halves, axis=1)

    pairs1 = hy // 2

    def layer1(i, carry):
        x = i // pairs1
        y = 2 * lax.rem(i, pairs1)
        both = jnp.dot(w1t[...], stacked(a1, x, y), preferred_element_type=F32)
        hidden, slope = gelu_pair(both[0:chan])
        gx_cell = ix * dx + x - 1
        gy_cell = iy * dy + y - 2
        inside = jnp.logical_and(
            jnp.logical_and(gx_cell >= 0, gx_cell < nx * dx), jnp.logical_and(gy_cell >= 0, gy_cell < ny * dy)
        )
        keep = inside.astype(F32)
        tangent = (keep * (slope * both[chan : 2 * chan])).astype(BF16)
        hidden = (keep * hidden).astype(BF16)
        fields = [carry[0:2], carry[2:4]]
        for half in range(2):
            cols = slice(128 * half, 128 * half + 128)
            for f, value in enumerate((tangent, hidden)):
                a2[f, x, y + half, chan : 2 * chan, :] = value[:, cols]
                fields[f] = packed(value[:, cols], x * hy + y + half, fields[f])
            slope_ref[x, y + half] = slope[:, cols]
        return (*fields[0], *fields[1])

    edges = lax.fori_loop(0, hx * pairs1, layer1, (blank,) * 4, unroll=2)
    pk2[0, 0], pk2[1, 0], pk2[0, 1], pk2[1, 1] = edges

    def send_hid(n, oz):
        return pltpu.make_async_remote_copy(
            pk2.at[n], ed2.at[1 - n], xs2.at[n], xr2.at[n], device_id=at(0, 0, oz), device_id_type=MESH
        )

    for n, oz in enumerate((-1, 1)):
        @pl.when(there(0, 0, oz))
        def _():
            send_hid(n, oz).start()
    for n, oz in enumerate((-1, 1)):
        @pl.when(there(0, 0, -oz))
        def _():
            send_hid(n, oz).wait_recv()

    def slab2(i, _):
        x = i // hy
        y = lax.rem(i, hy)
        for f in range(2):
            before, after = shifted(a2[f, x, y, chan : 2 * chan, :], ed2[0, f], ed2[1, f], i)
            a2[f, x, y, 0:chan, :] = before
            a2[f, x, y, 2 * chan : 3 * chan, :] = after
        return 0

    lax.fori_loop(0, hx * hy, slab2, 0, unroll=2)

    pairs2 = (dy + 2) // 2

    def layer2(i, carry):
        x = i // pairs2
        y = 2 * lax.rem(i, pairs2)
        both = jnp.concatenate([stacked(a2.at[0], x, y), stacked(a2.at[1], x, y)], axis=0)
        out = jnp.dot(w2t[...], both, preferred_element_type=F32)
        for half in range(2):
            gy_cell = iy * dy + y + half - 1
            keep = jnp.logical_and(gy_cell >= 0, gy_cell < ny * dy).astype(F32)
            value = (keep * out[:, 128 * half : 128 * half + 128]).astype(BF16)
            a3[x + 1, y + half, chan : 2 * chan, :] = value
            carry = packed(value, x * (dy + 2) + y + half, carry)
        return carry

    pk3[0], pk3[1] = lax.fori_loop(0, dx * pairs2, layer2, (blank, blank), unroll=2)

    def send_plane(n, ox):
        return pltpu.make_async_remote_copy(
            a3.at[1 if ox < 0 else dx, :, chan : 2 * chan, :],
            a3.at[dx + 1 if ox < 0 else 0, :, chan : 2 * chan, :],
            ps3.at[n], pr3.at[n], device_id=at(ox, 0, 0), device_id_type=MESH,
        )

    def send_jv(n):
        ox, oz = SIDES[n]
        return pltpu.make_async_remote_copy(
            pk3.at[1 if oz > 0 else 0], ed3.at[0 if oz > 0 else 1, 1 - ox],
            xs3.at[n], xr3.at[n], device_id=at(ox, 0, oz), device_id_type=MESH,
        )

    for n, ox in enumerate((-1, 1)):
        @pl.when(there(ox, 0, 0))
        def _():
            send_plane(n, ox).start()
    for n, (ox, oz) in enumerate(SIDES):
        @pl.when(there(ox, 0, oz))
        def _():
            send_jv(n).start()

    for x in range(dx):
        own = a3[x + 1, 1 : 1 + dy, chan : 2 * chan, :]
        ej[x, 3 : 3 + dy] = own
        jv_out[x] = own

    def correlate(read, e_ref):
        total = None
        for x in range(dx):
            lhs = jnp.concatenate(
                [
                    jnp.concatenate([read(x + kx, q) for kx in range(3)], axis=0)
                    for q in range(dy + 2)
                ],
                axis=1,
            )
            rhs = jnp.concatenate(
                [
                    jnp.concatenate([e_ref[x, q - ky + 3] for ky in range(4)], axis=0)
                    for q in range(dy + 2)
                ],
                axis=1,
            )
            product = lax.dot_general(lhs, rhs, (((1,), (1,)), ((), ())), preferred_element_type=F32)
            total = product if total is None else total + product
        return total

    lane8 = lax.broadcasted_iota(jnp.int32, (8, 128), 1)

    def put_part(f, value):
        for t in range(nz * tiles):
            if t < 27:
                j, s = t // 9, t % 9
                tail = pltpu.roll(value[216 + 8 * s : 224 + 8 * s], 96 - 32 * j, 1)
                part[t // tiles, f, t % tiles] = jnp.where(lane8 < 96, value[8 * t : 8 * t + 8], tail)
            else:
                part[t // tiles, f, t % tiles] = jnp.zeros((8, 128), F32)

    def send1(f, d):
        peer = z_peer(d)
        return pltpu.make_async_remote_copy(
            part.at[peer["gz"], f], recv1.at[d - 1, f], s1.at[f, d - 1], r1.at[f, d - 1],
            device_id=peer, device_id_type=MESH,
        )

    put_part(0, correlate(lambda x, q: a2[1, x, q + 1], ej))
    for d in range(1, nz):
        send1(0, d).start()

    for n, ox in enumerate((-1, 1)):
        @pl.when(there(-ox, 0, 0))
        def _():
            send_plane(n, ox).wait_recv()
    for n, (ox, oz) in enumerate(SIDES):
        @pl.when(there(-ox, 0, -oz))
        def _():
            send_jv(n).wait_recv()

    def slab3(i, _):
        x = i // (dy + 2)
        y = lax.rem(i, dy + 2)
        bx = (x + dx - 1) // dx
        j = lax.rem(x + dx - 1, dx) * (dy + 2) + y
        before, after = shifted(a3[x, y, chan : 2 * chan, :], ed3[0, bx], ed3[1, bx], j)
        a3[x, y, 0:chan, :] = before
        a3[x, y, 2 * chan : 3 * chan, :] = after
        return 0

    lax.fori_loop(0, hx * (dy + 2), slab3, 0, unroll=4)

    pairs3 = dy // 2

    def layer3(i, _):
        x = i // pairs3
        y = 2 * lax.rem(i, pairs3)
        out = jnp.dot(w3t[...], stacked(a3, x, y), preferred_element_type=F32)
        for half in range(2):
            value = slope_ref[x + 1, y + half + 2] * out[:, 128 * half : 128 * half + 128]
            eb[x, y + half + 3] = value.astype(BF16)
        return 0

    lax.fori_loop(0, dx * pairs3, layer3, 0, unroll=2)

    put_part(1, correlate(lambda x, q: a1[x + 1, q + 2], eb))
    for d in range(1, nz):
        send1(1, d).start()

    for f in range(2):
        total = part[iz, f]
        for d in range(1, nz):
            send1(f, d).wait_recv()
            total = total + recv1[d - 1, f]
        for r in range(plane * share):
            if r < 8 * tiles:
                rows[r // share, f * share + r % share : f * share + r % share + 1, :] = total[r // 8, r % 8 : r % 8 + 1, :]
            else:
                rows[r // share, f * share + r % share : f * share + r % share + 1, :] = jnp.zeros((1, 128), F32)

    def send2(d):
        q, peer = p_peer(d)
        return pltpu.make_async_remote_copy(
            rows.at[q], recv2.at[d - 1], s2.at[d - 1], r2.at[d - 1], device_id=peer, device_id_type=MESH
        )

    def send3(d):
        q, peer = p_peer(d)
        return pltpu.make_async_remote_copy(
            gath.at[me], gath.at[me], s3.at[d - 1], r3.at[d - 1], device_id=peer, device_id_type=MESH
        )

    def start2(d, _):
        send2(d).start()
        return 0

    def take2(d, acc):
        send2(d).wait_recv()
        return acc + recv2[d - 1]

    def start3(d, _):
        send3(d).start()
        return 0

    def take3(d, _):
        send3(d).wait_recv()
        return 0

    lax.fori_loop(1, plane, start2, 0)
    gath[me] = lax.fori_loop(1, plane, take2, rows[me])
    lax.fori_loop(1, plane, start3, 0)
    lax.fori_loop(1, plane, take3, 0)
    for f in range(2):
        for r in range(8 * tiles):
            chunk[f, r // 8, r % 8 : r % 8 + 1, :] = gath[r // share, f * share + r % share : f * share + r % share + 1, :]

    def send4(d):
        return pltpu.make_async_remote_copy(
            chunk, tot.at[iz], s4.at[d - 1], r4.at[d - 1], device_id=z_peer(d), device_id_type=MESH
        )

    for d in range(1, nz):
        send4(d).start()
    tot[iz] = chunk[...]
    for d in range(1, nz):
        send4(d).wait_recv()

    for n, o in enumerate(OFFSETS):
        @pl.when(there(*o))
        def _():
            send_vol(n).wait_send()
    for n, oz in enumerate((-1, 1)):
        @pl.when(there(0, 0, oz))
        def _():
            send_hid(n, oz).wait_send()
    for n, ox in enumerate((-1, 1)):
        @pl.when(there(ox, 0, 0))
        def _():
            send_plane(n, ox).wait_send()
    for n, (ox, oz) in enumerate(SIDES):
        @pl.when(there(ox, 0, oz))
        def _():
            send_jv(n).wait_send()
    for d in range(1, nz):
        send1(0, d).wait_send()
        send1(1, d).wait_send()
        send4(d).wait_send()

    def drain(d, _):
        send2(d).wait_send()
        send3(d).wait_send()
        return 0

    lax.fori_loop(1, plane, drain, 0)


def last_kernel(tiles, count_all, factor, tot, jv_raw, v_first, v_second, jv, gv_first, gv_second):
    for x in range(jv_raw.shape[0]):
        jv[:, x] = jnp.transpose(jv_raw[x], (1, 0, 2))
    for f, (v_ref, out) in enumerate(((v_second, gv_second), (v_first, gv_first))):
        tile = [tot[t // tiles, f, t % tiles] for t in range(27)]
        for kx in range(3):
            for ky in range(3):
                pieces = []
                for u in range(12 * kx, 12 * kx + 12):
                    if u < 27:
                        piece = tile[u] if ky == 0 else pltpu.roll(tile[u], 128 - 32 * ky, 1)
                    else:
                        piece = pltpu.roll(tile[9 * ky + u - 27], 32, 1)
                    pieces.append(piece[:, 0:32])
                k = 3 * kx + ky
                summed = jnp.concatenate(pieces, axis=0)
                base = v_ref[96 * k : 96 * k + 96, :].astype(F32)
                out[k] = factor * (summed / count_all + 0.1 * base)


def body(volume, w_first, w_second, v_first, v_second):
    chan, dx, dy, dz = volume.shape
    nx, ny, nz = lax.axis_size("gx"), lax.axis_size("gy"), lax.axis_size("gz")
    plane = nx * ny
    tiles = -(-27 // nz)
    share = -(-8 * tiles // plane)
    count_all = float(dx * dy * dz * nx * ny * nz)
    factor = math.sqrt(27.0 * chan)
    shape = w_first.shape
    flat = [w.reshape(27 * chan, chan) for w in (w_first, w_second, v_first, v_second)]
    vm = pl.BlockSpec(memory_space=pltpu.VMEM)
    dma = pltpu.SemaphoreType.DMA
    tot, jv_raw = pl.pallas_call(
        functools.partial(main_kernel, nx, ny, nz, dx, dy, tiles, share),
        out_shape=(
            jax.ShapeDtypeStruct((nz, 2, tiles, 8, 128), F32),
            jax.ShapeDtypeStruct((dx, dy, chan, 128), BF16),
        ),
        in_specs=[vm] * 5,
        out_specs=(vm, vm),
        scratch_shapes=[
            pltpu.VMEM((3 * dx, dy + 6, 3 * chan, 128), BF16),
            pltpu.VMEM((2, dx + 2, dy + 4, 3 * chan, 128), BF16),
            pltpu.VMEM((dx + 2, dy + 2, 3 * chan, 128), BF16),
            pltpu.VMEM((dx + 2, dy + 4, chan, 128), F32),
            pltpu.VMEM((dx, dy + 5, chan, 128), BF16),
            pltpu.VMEM((dx, dy + 5, chan, 128), BF16),
            pltpu.VMEM((2 * chan, 896), BF16),
            pltpu.VMEM((chan, 1792), BF16),
            pltpu.VMEM((chan, 896), BF16),
            pltpu.VMEM((2, chan, 128), BF16),
            pltpu.VMEM((2, 3, 3, chan, 128), BF16),
            pltpu.VMEM((2, 2, chan, 128), BF16),
            pltpu.VMEM((2, 2, chan, 128), BF16),
            pltpu.VMEM((2, chan, 128), BF16),
            pltpu.VMEM((2, 3, chan, 128), BF16),
            pltpu.VMEM((nz, 2, tiles, 8, 128), F32),
            pltpu.VMEM((nz - 1, 2, tiles, 8, 128), F32),
            pltpu.VMEM((plane, 2 * share, 128), F32),
            pltpu.VMEM((plane - 1, 2 * share, 128), F32),
            pltpu.VMEM((plane, 2 * share, 128), F32),
            pltpu.VMEM((2, tiles, 8, 128), F32),
            dma((26,)), dma((26,)),
            dma((2,)), dma((2,)),
            dma((6,)), dma((6,)),
            dma((2,)), dma((2,)),
            dma((2, nz - 1)), dma((2, nz - 1)),
            dma((plane - 1,)), dma((plane - 1,)),
            dma((plane - 1,)), dma((plane - 1,)),
            dma((nz - 1,)), dma((nz - 1,)),
        ],
        compiler_params=pltpu.CompilerParams(collective_id=0, has_side_effects=True),
        cost_estimate=pl.CostEstimate(flops=2000000000, bytes_accessed=2000000, transcendentals=400000),
    )(volume, *flat)
    jv, gv_first, gv_second = pl.pallas_call(
        functools.partial(last_kernel, tiles, count_all, factor),
        out_shape=(
            jax.ShapeDtypeStruct((chan, dx, dy, 128), BF16),
            jax.ShapeDtypeStruct((9, 3 * chan, chan), F32),
            jax.ShapeDtypeStruct((9, 3 * chan, chan), F32),
        ),
        in_specs=[vm] * 4,
        out_specs=(vm, vm, vm),
    )(tot, jv_raw, flat[2], flat[3])
    return (jv, gv_first.reshape(shape), gv_second.reshape(shape))


def solution(mesh):
    in_specs = (P(None, "gx", "gy", "gz"), P(), P(), P(), P())
    out_specs = (P(None, "gx", "gy", "gz"), P(), P())
    return jax.shard_map(body, mesh=mesh, in_specs=in_specs, out_specs=out_specs, check_vma=False)
```

```python
import functools
import itertools
import math

import jax
import jax.numpy as jnp
from jax import lax
from jax.experimental import pallas as pl
from jax.experimental.pallas import tpu as pltpu
from jax.sharding import PartitionSpec as P

MESH = pl.DeviceIdType.MESH
BF16 = jnp.bfloat16
F32 = jnp.float32
OFFSETS = [o for o in itertools.product((-1, 0, 1), repeat=3) if o != (0, 0, 0)]
VOLUME = [((ox, 0, 0), False) for ox in (-1, 1)]
VOLUME += [((ox, 0, oz), False) for ox in (0, -1, 1) for oz in (-1, 1)]
VOLUME += [(o, False) for o in OFFSETS if o[1] != 0]
VOLUME += [((ox, 0, 0), True) for ox in (-1, 1)]
SIDES = [(ox, oz) for ox in (-1, 0, 1) for oz in (-1, 1)]


def gelu_pair(pre):
    square = pre * pre
    hyper = jnp.tanh(0.7978845608 * (pre + 0.044715 * square * pre))
    half = 0.5 * (1.0 + hyper)
    hidden = pre * half
    slope = half + (0.5 * pre) * (1.0 - hyper * hyper) * (0.7978845608 * (1.0 + 0.134145 * square))
    return (hidden, slope)


def main_kernel(
    nx, ny, nz, dx, dy, tiles, share,
    vol, w_first, w_second, v_first, v_second,
    tot, jv_out,
    r1, q1, r2, q2, r3, q3, slope_ref, acc3, ej, eb, w1t, w2t, w3t,
    pk1, ed1, pk2, ed2, pk3, ed3,
    part, recv1, rows, recv2, gath, chunk,
    xs1, xr1, xs2, xr2, xs3, xr3, ps3, pr3,
    as1, ar1, as2, ar2, as3, ar3, as4, ar4,
):
    ix, iy, iz = lax.axis_index("gx"), lax.axis_index("gy"), lax.axis_index("gz")
    me = iy * nx + ix
    chan = vol.shape[0]
    two = 2 * chan
    hx, hy = dx + 2, dy + 4
    lane = lax.broadcasted_iota(jnp.int32, (chan, 128), 1)

    def there(ox, oy, oz):
        ok = None
        for offset, index, count in ((ox, ix, nx), (oy, iy, ny), (oz, iz, nz)):
            if offset:
                one = index < count - 1 if offset > 0 else index > 0
                ok = one if ok is None else jnp.logical_and(ok, one)
        return ok

    def at(ox, oy, oz):
        return {"gx": ix + ox, "gy": iy + oy, "gz": iz + oz}

    zs = [lax.rem(iz + d, nz) for d in range(nz)]
    ys = [lax.rem(iy + d, ny) for d in range(ny)]
    xs = [lax.rem(ix + d, nx) for d in range(nx)]
    turns = [(ey, ex) for ey in range(ny) for ex in range(nx)][1:]

    def z_peer(d):
        return {"gx": ix, "gy": iy, "gz": zs[d]}

    def p_peer(n):
        ey, ex = turns[n]
        return {"gx": xs[ex], "gy": ys[ey], "gz": iz}

    def copy(src, dst, send, recv, peer):
        return pltpu.make_async_remote_copy(src, dst, send, recv, device_id=peer, device_id_type=MESH)

    def guarded(cond, action):
        @pl.when(cond)
        def _():
            action()

    barrier = pltpu.get_barrier_semaphore()

    def greet(peer):
        pl.semaphore_signal(barrier, inc=1, device_id=peer, device_id_type=MESH)

    for n in range(len(turns)):
        greet(p_peer(n))
    for o in OFFSETS:
        guarded(there(*o), lambda: greet(at(*o)))
    for d in range(1, nz):
        greet(z_peer(d))

    def zero(ref):
        ref[...] = jnp.zeros(ref.shape, ref.dtype)

    for x in range(dx):
        r1[dx + x, 3 : 3 + dy] = jnp.transpose(vol[:, x], (1, 0, 2))

    def packed(raw, j, pair):
        first = jnp.where(lane == j, jnp.broadcast_to(raw[:, 0:1], raw.shape), pair[0])
        last = jnp.where(lane == j, jnp.broadcast_to(raw[:, 127:128], raw.shape), pair[1])
        return first, last

    blank = jnp.zeros((chan, 128), BF16)
    edges = (blank, blank)
    for x in range(dx):
        for y in range(dy):
            edges = packed(r1[dx + x, 3 + y], x * dy + y, edges)
    pk1[0], pk1[1] = edges

    @pl.when(ix == 0)
    def _():
        zero(r1.at[0:dx])
        zero(ed1.at[:, 0])
        zero(r3.at[0])
        zero(ed3.at[:, 0])

    @pl.when(ix == nx - 1)
    def _():
        zero(r1.at[2 * dx : 3 * dx])
        zero(ed1.at[:, 2])
        zero(r3.at[dx + 1])
        zero(ed3.at[:, 2])

    @pl.when(iy == 0)
    def _():
        zero(r1.at[:, 0:3])
        zero(ed1.at[:, :, 0])

    @pl.when(iy == ny - 1)
    def _():
        zero(r1.at[:, 3 + dy : 6 + dy])
        zero(ed1.at[:, :, 2])

    @pl.when(iz == 0)
    def _():
        zero(ed1.at[0])
        zero(ed2.at[0])
        zero(ed3.at[0])

    @pl.when(iz == nz - 1)
    def _():
        zero(ed1.at[1])
        zero(ed2.at[1])
        zero(ed3.at[1])

    def span(index, count):
        return 3 - (index == 0).astype(jnp.int32) - (index == count - 1).astype(jnp.int32)

    near = span(ix, nx) * span(iy, ny) * span(iz, nz) - 1
    pl.semaphore_wait(barrier, near + nz - 1 + len(turns))

    def send_vol(n):
        (ox, oy, oz), far = VOLUME[n]
        if oz:
            src = pk1.at[1 if oz > 0 else 0]
            dst = ed1.at[0 if oz > 0 else 1, 1 - ox, 1 - oy]
        elif oy == 0:
            own = dx if (ox < 0) != far else 2 * dx - 1
            to = own - dx * ox
            src = r1.at[own, 3 : 3 + dy]
            dst = r1.at[to, 3 : 3 + dy]
        else:
            src_y = 3 if oy < 0 else dy
            dst_y = 0 if oy > 0 else 3 + dy
            to = dx * (1 - ox)
            src = r1.at[dx : 2 * dx, src_y : src_y + 3]
            dst = r1.at[to : to + dx, dst_y : dst_y + 3]
        return copy(src, dst, xs1.at[n], xr1.at[n], at(ox, oy, oz))

    def back(o):
        return there(*(-c for c in o))

    for n, (o, _) in enumerate(VOLUME):
        guarded(there(*o), lambda: send_vol(n).start())

    def take_vol(test):
        for n, (o, far) in enumerate(VOLUME):
            if test(o, far):
                guarded(back(o), lambda: send_vol(n).wait_recv())

    taps = w_first.shape[0]
    third = taps // 3
    w1t[0:chan, :] = w_first[...].T
    w1t[chan:two, :] = v_first[...].T
    for f, w_ref in enumerate((w_second, v_second)):
        turned = w_ref[...].T
        for kx in range(3):
            w2t[chan * (2 - kx) : chan * (3 - kx), third * f : third * (f + 1)] = turned[:, third * kx : third * (kx + 1)]
    for k in range(27):
        kx, rest = k // 9, k % 9
        w3t[chan * (2 - kx) : chan * (3 - kx), chan * rest : chan * (rest + 1)] = w_second[chan * (26 - k) : chan * (27 - k), :]
    for x in range(dx):
        zero(ej.at[x, 0:3])
        zero(ej.at[x, 3 + dy : 5 + dy])
        zero(eb.at[x, 0:3])
        zero(eb.at[x, 3 + dy : 5 + dy])

    def shift(raw_ref, out_ref, x, y, left, right, j):
        raw = raw_ref[x, y]
        before = left if j == 0 else pltpu.roll(left, 128 - j, 1)
        after = right if j == 127 else pltpu.roll(right, 127 - j, 1)
        out_ref[x, y, 0:chan] = jnp.where(lane == 0, before, pltpu.roll(raw, 1, 1))
        out_ref[x, y, chan:two] = jnp.where(lane == 127, after, pltpu.roll(raw, 127, 1))

    def slab1(planes, lines):
        for x in planes:
            for y in lines:
                bx, by = x // dx, (y + dy - 3) // dy
                shift(r1, q1, x, y, ed1[0, bx, by], ed1[1, bx, by], (x % dx) * dy + (y + dy - 3) % dy)

    def three(raw_ref, out_ref, x, y):
        return [out_ref[x, y, 0:chan], raw_ref[x, y], out_ref[x, y, chan:two]]

    def layer1(x, y, carry):
        halves = []
        for half in range(2):
            pieces = []
            for kx in range(3):
                for ky in range(3):
                    pieces += three(r1, q1, x + kx, y + half + ky)
            halves.append(jnp.concatenate(pieces, axis=0))
        both = jnp.dot(w1t[...], jnp.concatenate(halves, axis=1), preferred_element_type=F32)
        hidden, slope = gelu_pair(both[0:chan])
        gx_cell = ix * dx + x - 1
        gy_cell = iy * dy + y - 2
        inside = jnp.logical_and(
            jnp.logical_and(gx_cell >= 0, gx_cell < nx * dx), jnp.logical_and(gy_cell >= 0, gy_cell < ny * dy)
        )
        keep = inside.astype(F32)
        tangent = (keep * (slope * both[chan:two])).astype(BF16)
        hidden = (keep * hidden).astype(BF16)
        fields = [carry[0:2], carry[2:4]]
        for half in range(2):
            cols = slice(128 * half, 128 * half + 128)
            for f, value in enumerate((tangent, hidden)):
                r2[f, x, y + half] = value[:, cols]
                fields[f] = packed(value[:, cols], x * hy + y + half, fields[f])
            slope_ref[x, y + half] = slope[:, cols]
        return (*fields[0], *fields[1])

    own_y = range(3, 3 + dy)
    halo_y = [*range(3), *range(3 + dy, 6 + dy)]
    inner = (dy - 4) // 2
    take_vol(lambda o, far: o[0] == 0 and o[1] == 0)
    slab1(range(dx, 2 * dx), own_y)
    take_vol(lambda o, far: o[0] != 0 and o[1] == 0 and not far)
    slab1((dx - 1, 2 * dx), own_y)
    edges = lax.fori_loop(
        0, dx * inner, lambda i, c: layer1(1 + i // inner, 4 + 2 * lax.rem(i, inner), c), (blank,) * 4, unroll=4
    )
    take_vol(lambda o, far: far)
    slab1((0, 3 * dx - 1), own_y)
    edges = lax.fori_loop(
        0, 2 * inner, lambda i, c: layer1((hx - 1) * (i // inner), 4 + 2 * lax.rem(i, inner), c), edges, unroll=4
    )
    take_vol(lambda o, far: o[1] != 0)
    slab1(range(3 * dx), halo_y)

    def outer(i, c):
        k = lax.rem(i, 4)
        return layer1(i // 4, 2 * lax.rem(k, 2) + dy * (k // 2), c)

    edges = lax.fori_loop(0, hx * 4, outer, edges, unroll=4)
    pk2[0, 0], pk2[1, 0], pk2[0, 1], pk2[1, 1] = edges

    def send_hid(n, oz):
        return copy(pk2.at[n], ed2.at[1 - n], xs2.at[n], xr2.at[n], at(0, 0, oz))

    for n, oz in enumerate((-1, 1)):
        guarded(there(0, 0, oz), lambda: send_hid(n, oz).start())
    for n, oz in enumerate((-1, 1)):
        guarded(there(0, 0, -oz), lambda: send_hid(n, oz).wait_recv())

    for f in range(2):
        for x in range(hx):
            for y in range(hy):
                shift(r2.at[f], q2.at[f], x, y, ed2[0, f], ed2[1, f], x * hy + y)

    def layer2(pair, carry):
        y = 2 * pair
        out = [None] * dx
        for x in range(hx):
            halves = []
            for half in range(2):
                pieces = []
                for f in range(2):
                    for ky in range(3):
                        pieces += three(r2.at[f], q2.at[f], x, y + half + ky)
                halves.append(jnp.concatenate(pieces, axis=0))
            low, high = max(0, x - 2), min(dx - 1, x)
            left = w2t[chan * (2 - x + low) : chan * (3 - x + high), :]
            product = jnp.dot(left, jnp.concatenate(halves, axis=1), preferred_element_type=F32)
            for to in range(low, high + 1):
                term = product[chan * (to - low) : chan * (to - low + 1)]
                out[to] = term if out[to] is None else out[to] + term
        for x in range(dx):
            for half in range(2):
                gy_cell = iy * dy + y + half - 1
                keep = jnp.logical_and(gy_cell >= 0, gy_cell < ny * dy).astype(F32)
                value = (keep * out[x][:, 128 * half : 128 * half + 128]).astype(BF16)
                r3[x + 1, y + half] = value
                carry = packed(value, x * (dy + 2) + y + half, carry)
        return carry

    cut = 2 * ((dy + 2 + 2) // 4)

    def send_plane(n, ox, late):
        lines = slice(cut, dy + 2) if late else slice(0, cut)
        return copy(
            r3.at[1 if ox < 0 else dx, lines], r3.at[dx + 1 if ox < 0 else 0, lines],
            ps3.at[n, int(late)], pr3.at[n, int(late)], at(ox, 0, 0),
        )

    def send_jv(n):
        ox, oz = SIDES[n]
        return copy(pk3.at[1 if oz > 0 else 0], ed3.at[0 if oz > 0 else 1, 1 - ox], xs3.at[n], xr3.at[n], at(ox, 0, oz))

    edges = lax.fori_loop(0, cut // 2, layer2, (blank, blank), unroll=cut // 2)
    for n, ox in enumerate((-1, 1)):
        guarded(there(ox, 0, 0), lambda: send_plane(n, ox, False).start())
    rest = (dy + 2 - cut) // 2
    pk3[0], pk3[1] = lax.fori_loop(0, rest, lambda i, c: layer2(cut // 2 + i, c), edges, unroll=rest)
    for n, (ox, oz) in enumerate(SIDES):
        guarded(there(ox, 0, oz), lambda: send_jv(n).start())
    for n, ox in enumerate((-1, 1)):
        guarded(there(ox, 0, 0), lambda: send_plane(n, ox, True).start())

    for x in range(dx):
        own = r3[x + 1, 1 : 1 + dy]
        ej[x, 3 : 3 + dy] = own
        jv_out[x] = own

    def correlate(raw_ref, out_ref, x0, y0, e_ref):
        total = None
        for x in range(dx):
            lhs, rhs = [], []
            for q in range(dy + 2):
                pieces = []
                for kx in range(3):
                    pieces += three(raw_ref, out_ref, x + kx + x0, q + y0)
                lhs.append(jnp.concatenate(pieces, axis=0))
                rhs.append(jnp.concatenate([e_ref[x, q - ky + 3] for ky in range(4)], axis=0))
            product = lax.dot_general(
                jnp.concatenate(lhs, axis=1), jnp.concatenate(rhs, axis=1),
                (((1,), (1,)), ((), ())), preferred_element_type=F32,
            )
            total = product if total is None else total + product
        return total

    lane8 = lax.broadcasted_iota(jnp.int32, (8, 128), 1)

    def put_part(f, value):
        for t in range(nz * tiles):
            if t < 27:
                j, s = t // 9, t % 9
                tail = pltpu.roll(value[216 + 8 * s : 224 + 8 * s], 96 - 32 * j, 1)
                part[t // tiles, f, t % tiles] = jnp.where(lane8 < 96, value[8 * t : 8 * t + 8], tail)
            else:
                part[t // tiles, f, t % tiles] = jnp.zeros((8, 128), F32)

    def send1(f, d):
        return copy(part.at[zs[d], f], recv1.at[d - 1, f], as1.at[f, d - 1], ar1.at[f, d - 1], z_peer(d))

    put_part(0, correlate(r2.at[1], q2.at[1], 0, 1, ej))
    for d in range(1, nz):
        send1(0, d).start()

    def take_jv(own):
        for n, (ox, oz) in enumerate(SIDES):
            if (ox == 0) == own:
                guarded(there(-ox, 0, -oz), lambda: send_jv(n).wait_recv())

    def slab3(planes):
        for x in planes:
            bx = (x + dx - 1) // dx
            for y in range(dy + 2):
                shift(r3, q3, x, y, ed3[0, bx], ed3[1, bx], ((x + dx - 1) % dx) * (dy + 2) + y)

    def layer3(x, y):
        halves = []
        for half in range(2):
            pieces = []
            for ky in range(3):
                pieces += three(r3, q3, x, y + half + ky)
            halves.append(jnp.concatenate(pieces, axis=0))
        low, high = max(0, x - 2), min(dx - 1, x)
        left = w3t[chan * (2 - x + low) : chan * (3 - x + high), :]
        product = jnp.dot(left, jnp.concatenate(halves, axis=1), preferred_element_type=F32)
        return {to: product[chan * (to - low) : chan * (to - low + 1)] for to in range(low, high + 1)}

    take_jv(True)
    slab3(range(1, dx + 1))

    def own3(pair, _):
        y = 2 * pair
        parts = [layer3(x, y) for x in range(1, dx + 1)]
        for x in range(dx):
            summed = parts[0][x] + parts[1][x]
            for half in range(2):
                acc3[x, y + half] = summed[:, 128 * half : 128 * half + 128]
        return 0

    lax.fori_loop(0, dy // 2, own3, 0, unroll=4)
    take_jv(False)
    for n, ox in enumerate((-1, 1)):
        for late in (False, True):
            guarded(there(-ox, 0, 0), lambda: send_plane(n, ox, late).wait_recv())
    slab3((0, dx + 1))

    def halo3(pair, _):
        y = 2 * pair
        for x, plane_x in ((0, 0), (dx - 1, dx + 1)):
            term = layer3(plane_x, y)[x]
            for half in range(2):
                cols = slice(128 * half, 128 * half + 128)
                value = slope_ref[x + 1, y + half + 2] * (acc3[x, y + half] + term[:, cols])
                eb[x, y + half + 3] = value.astype(BF16)
        return 0

    lax.fori_loop(0, dy // 2, halo3, 0, unroll=4)

    put_part(1, correlate(r1, q1, 1, 2, eb))
    for d in range(1, nz):
        send1(1, d).start()

    for f in range(2):
        total = part[iz, f]
        for d in range(1, nz):
            send1(f, d).wait_recv()
            total = total + recv1[d - 1, f]
        for r in range(nx * ny * share):
            slot = slice(f * share + r % share, f * share + r % share + 1)
            if r < 8 * tiles:
                rows[r // share, slot, :] = total[r // 8, r % 8 : r % 8 + 1, :]
            else:
                rows[r // share, slot, :] = jnp.zeros((1, 128), F32)

    def send2(n):
        ey, ex = turns[n]
        return copy(rows.at[ys[ey] * nx + xs[ex]], recv2.at[n], as2.at[n], ar2.at[n], p_peer(n))

    def send3(n):
        return copy(gath.at[me], gath.at[me], as3.at[n], ar3.at[n], p_peer(n))

    for n in range(len(turns)):
        send2(n).start()
    total = rows[me]
    for n in range(len(turns)):
        send2(n).wait_recv()
        total = total + recv2[n]
    gath[me] = total
    for n in range(len(turns)):
        send3(n).start()
    for n in range(len(turns)):
        send3(n).wait_recv()
    for f in range(2):
        for r in range(8 * tiles):
            slot = slice(f * share + r % share, f * share + r % share + 1)
            chunk[f, r // 8, r % 8 : r % 8 + 1, :] = gath[r // share, slot, :]

    def send4(d):
        return copy(chunk, tot.at[iz], as4.at[d - 1], ar4.at[d - 1], z_peer(d))

    for d in range(1, nz):
        send4(d).start()
    tot[iz] = chunk[...]
    for d in range(1, nz):
        send4(d).wait_recv()

    for n, (o, _) in enumerate(VOLUME):
        guarded(there(*o), lambda: send_vol(n).wait_send())
    for n, oz in enumerate((-1, 1)):
        guarded(there(0, 0, oz), lambda: send_hid(n, oz).wait_send())
    for n, ox in enumerate((-1, 1)):
        for late in (False, True):
            guarded(there(ox, 0, 0), lambda: send_plane(n, ox, late).wait_send())
    for n, (ox, oz) in enumerate(SIDES):
        guarded(there(ox, 0, oz), lambda: send_jv(n).wait_send())
    for d in range(1, nz):
        send1(0, d).wait_send()
        send1(1, d).wait_send()
        send4(d).wait_send()
    for n in range(len(turns)):
        send2(n).wait_send()
        send3(n).wait_send()


def last_kernel(tiles, count_all, factor, tot, jv_raw, v_first, v_second, jv, gv_first, gv_second):
    for x in range(jv_raw.shape[0]):
        jv[:, x] = jnp.transpose(jv_raw[x], (1, 0, 2))
    for f, (v_ref, out) in enumerate(((v_second, gv_second), (v_first, gv_first))):
        tile = [tot[t // tiles, f, t % tiles] for t in range(27)]
        for kx in range(3):
            for ky in range(3):
                pieces = []
                for u in range(12 * kx, 12 * kx + 12):
                    if u < 27:
                        piece = tile[u] if ky == 0 else pltpu.roll(tile[u], 128 - 32 * ky, 1)
                    else:
                        piece = pltpu.roll(tile[9 * ky + u - 27], 32, 1)
                    pieces.append(piece[:, 0:32])
                k = 3 * kx + ky
                summed = jnp.concatenate(pieces, axis=0)
                base = v_ref[96 * k : 96 * k + 96, :].astype(F32)
                out[k] = factor * (summed / count_all + 0.1 * base)


def body(volume, w_first, w_second, v_first, v_second):
    chan, dx, dy, dz = volume.shape
    nx, ny, nz = lax.axis_size("gx"), lax.axis_size("gy"), lax.axis_size("gz")
    plane = nx * ny
    tiles = -(-27 // nz)
    share = -(-8 * tiles // plane)
    count_all = float(dx * dy * dz * nx * ny * nz)
    factor = math.sqrt(27.0 * chan)
    shape = w_first.shape
    flat = [w.reshape(27 * chan, chan) for w in (w_first, w_second, v_first, v_second)]
    vm = pl.BlockSpec(memory_space=pltpu.VMEM)
    dma = pltpu.SemaphoreType.DMA
    tot, jv_raw = pl.pallas_call(
        functools.partial(main_kernel, nx, ny, nz, dx, dy, tiles, share),
        out_shape=(
            jax.ShapeDtypeStruct((nz, 2, tiles, 8, 128), F32),
            jax.ShapeDtypeStruct((dx, dy, chan, 128), BF16),
        ),
        in_specs=[vm] * 5,
        out_specs=(vm, vm),
        scratch_shapes=[
            pltpu.VMEM((3 * dx, dy + 6, chan, 128), BF16),
            pltpu.VMEM((3 * dx, dy + 6, 2 * chan, 128), BF16),
            pltpu.VMEM((2, dx + 2, dy + 4, chan, 128), BF16),
            pltpu.VMEM((2, dx + 2, dy + 4, 2 * chan, 128), BF16),
            pltpu.VMEM((dx + 2, dy + 2, chan, 128), BF16),
            pltpu.VMEM((dx + 2, dy + 2, 2 * chan, 128), BF16),
            pltpu.VMEM((dx + 2, dy + 4, chan, 128), F32),
            pltpu.VMEM((dx, dy, chan, 128), F32),
            pltpu.VMEM((dx, dy + 5, chan, 128), BF16),
            pltpu.VMEM((dx, dy + 5, chan, 128), BF16),
            pltpu.VMEM((2 * chan, 27 * chan), BF16),
            pltpu.VMEM((3 * chan, 18 * chan), BF16),
            pltpu.VMEM((3 * chan, 9 * chan), BF16),
            pltpu.VMEM((2, chan, 128), BF16),
            pltpu.VMEM((2, 3, 3, chan, 128), BF16),
            pltpu.VMEM((2, 2, chan, 128), BF16),
            pltpu.VMEM((2, 2, chan, 128), BF16),
            pltpu.VMEM((2, chan, 128), BF16),
            pltpu.VMEM((2, 3, chan, 128), BF16),
            pltpu.VMEM((nz, 2, tiles, 8, 128), F32),
            pltpu.VMEM((nz - 1, 2, tiles, 8, 128), F32),
            pltpu.VMEM((plane, 2 * share, 128), F32),
            pltpu.VMEM((plane - 1, 2 * share, 128), F32),
            pltpu.VMEM((plane, 2 * share, 128), F32),
            pltpu.VMEM((2, tiles, 8, 128), F32),
            dma((len(VOLUME),)), dma((len(VOLUME),)),
            dma((2,)), dma((2,)),
            dma((6,)), dma((6,)),
            dma((2, 2)), dma((2, 2)),
            dma((2, nz - 1)), dma((2, nz - 1)),
            dma((plane - 1,)), dma((plane - 1,)),
            dma((plane - 1,)), dma((plane - 1,)),
            dma((nz - 1,)), dma((nz - 1,)),
        ],
        compiler_params=pltpu.CompilerParams(collective_id=0, has_side_effects=True),
        cost_estimate=pl.CostEstimate(flops=2000000000, bytes_accessed=2000000, transcendentals=400000),
    )(volume, *flat)
    jv, gv_first, gv_second = pl.pallas_call(
        functools.partial(last_kernel, tiles, count_all, factor),
        out_shape=(
            jax.ShapeDtypeStruct((chan, dx, dy, 128), BF16),
            jax.ShapeDtypeStruct((9, 3 * chan, chan), F32),
            jax.ShapeDtypeStruct((9, 3 * chan, chan), F32),
        ),
        in_specs=[vm] * 4,
        out_specs=(vm, vm, vm),
    )(tot, jv_raw, flat[2], flat[3])
    return (jv, gv_first.reshape(shape), gv_second.reshape(shape))


def solution(mesh):
    in_specs = (P(None, "gx", "gy", "gz"), P(), P(), P(), P())
    out_specs = (P(None, "gx", "gy", "gz"), P(), P())
    return jax.shard_map(body, mesh=mesh, in_specs=in_specs, out_specs=out_specs, check_vma=False)
```

```python
import functools
import itertools
import math

import jax
import jax.numpy as jnp
from jax import lax
from jax.experimental import pallas as pl
from jax.experimental.pallas import tpu as pltpu
from jax.sharding import PartitionSpec as P

MESH = pl.DeviceIdType.MESH
BF16 = jnp.bfloat16
F32 = jnp.float32
OFFSETS = [o for o in itertools.product((-1, 0, 1), repeat=3) if o != (0, 0, 0)]
VOLUME = [(o, False) for o in OFFSETS if o[1] != 0 and o[2] == 0]
VOLUME += [(o, False) for o in OFFSETS if o[1] != 0 and o[2] != 0]
VOLUME += [((ox, 0, 0), False) for ox in (-1, 1)]
VOLUME += [((ox, 0, oz), False) for ox in (0, -1, 1) for oz in (-1, 1)]
VOLUME += [((ox, 0, 0), True) for ox in (-1, 1)]
SIDES = [(ox, oz) for ox in (-1, 0, 1) for oz in (-1, 1)]


def gelu_pair(pre):
    square = pre * pre
    hyper = jnp.tanh(0.7978845608 * (pre + 0.044715 * square * pre))
    half = 0.5 * (1.0 + hyper)
    hidden = pre * half
    slope = half + (0.5 * pre) * (1.0 - hyper * hyper) * (0.7978845608 * (1.0 + 0.134145 * square))
    return (hidden, slope)


def main_kernel(
    nx, ny, nz, dx, dy,
    vol_in, w_first_in, w_second_in, v_first_in, v_second_in,
    tot, jv_out,
    vol, w_first, w_second, v_first, v_second, load, r1, q1, r2, q2, r3, q3, slope_ref, acc3, ej, eb, w1t, w2t, w3t,
    pk1, ed1, pk2, ed2, pk3, ed3,
    part, recv_a, sum_a, recv_z, fin,
    xs1, xr1, xs2, xr2, xs3, xr3, ps3, pr3,
    sa, ra, sz, rz, sg, rg,
):
    ix, iy, iz = lax.axis_index("gx"), lax.axis_index("gy"), lax.axis_index("gz")
    me = iy * nx + ix
    chan = vol.shape[0]
    two = 2 * chan
    hx, hy = dx + 2, dy + 4
    lane = lax.broadcasted_iota(jnp.int32, (chan, 128), 1)

    def there(ox, oy, oz):
        ok = None
        for offset, index, count in ((ox, ix, nx), (oy, iy, ny), (oz, iz, nz)):
            if offset:
                one = index < count - 1 if offset > 0 else index > 0
                ok = one if ok is None else jnp.logical_and(ok, one)
        return ok

    def at(ox, oy, oz):
        return {"gx": ix + ox, "gy": iy + oy, "gz": iz + oz}

    wide = 4
    high = ny // wide
    planes = high * nx
    col, row = lax.rem(iy, wide), iy // wide
    level = row * nx + ix
    zs = [lax.rem(iz + d, nz) for d in range(nz)]
    cs = [lax.rem(col + d, wide) for d in range(wide)]
    turns = [(ez, ec) for ez in range(nz) for ec in range(wide)][1:]
    me = iz * wide + col

    def a_peer(n):
        ez, ec = turns[n]
        return {"gx": ix, "gy": row * wide + cs[ec], "gz": zs[ez]}

    def z_peer(d):
        other = lax.rem(level + d, planes)
        return {"gx": lax.rem(other, nx), "gy": (other // nx) * wide + col, "gz": iz}

    def copy(src, dst, send, recv, peer):
        return pltpu.make_async_remote_copy(src, dst, send, recv, device_id=peer, device_id_type=MESH)

    def guarded(cond, action):
        @pl.when(cond)
        def _():
            action()

    loads = [
        pltpu.make_async_copy(src, dst, load.at[n])
        for n, (src, dst) in enumerate(
            ((vol_in, vol), (w_first_in, w_first), (w_second_in, w_second), (v_first_in, v_first), (v_second_in, v_second))
        )
    ]
    for step in loads:
        step.start()
    barrier = pltpu.get_barrier_semaphore()

    def greet(peer):
        pl.semaphore_signal(barrier, inc=1, device_id=peer, device_id_type=MESH)

    for d in range(1, planes):
        greet(z_peer(d))
    for n in range(len(turns)):
        greet(a_peer(n))
    for o in OFFSETS:
        guarded(there(*o), lambda: greet(at(*o)))

    def zero(ref):
        ref[...] = jnp.zeros(ref.shape, ref.dtype)

    loads[0].wait()
    for x in range(dx):
        r1[dx + x, 3 : 3 + dy] = jnp.transpose(vol[:, x], (1, 0, 2))

    def packed(raw, j, pair):
        first = jnp.where(lane == j, jnp.broadcast_to(raw[:, 0:1], raw.shape), pair[0])
        last = jnp.where(lane == j, jnp.broadcast_to(raw[:, 127:128], raw.shape), pair[1])
        return first, last

    blank = jnp.zeros((chan, 128), BF16)
    edges = (blank, blank)
    for x in range(dx):
        for y in range(dy):
            edges = packed(r1[dx + x, 3 + y], x * dy + y, edges)
    pk1[0], pk1[1] = edges

    @pl.when(ix == 0)
    def _():
        zero(r1.at[0:dx])
        zero(ed1.at[:, 0])
        zero(r3.at[0])
        zero(ed3.at[:, 0])

    @pl.when(ix == nx - 1)
    def _():
        zero(r1.at[2 * dx : 3 * dx])
        zero(ed1.at[:, 2])
        zero(r3.at[dx + 1])
        zero(ed3.at[:, 2])

    @pl.when(iy == 0)
    def _():
        zero(r1.at[:, 0:3])
        zero(ed1.at[:, :, 0])

    @pl.when(iy == ny - 1)
    def _():
        zero(r1.at[:, 3 + dy : 6 + dy])
        zero(ed1.at[:, :, 2])

    @pl.when(iz == 0)
    def _():
        zero(ed1.at[0])
        zero(ed2.at[0])
        zero(ed3.at[0])

    @pl.when(iz == nz - 1)
    def _():
        zero(ed1.at[1])
        zero(ed2.at[1])
        zero(ed3.at[1])

    def span(index, count):
        return 3 - (index == 0).astype(jnp.int32) - (index == count - 1).astype(jnp.int32)

    near = span(ix, nx) * span(iy, ny) * span(iz, nz) - 1
    pl.semaphore_wait(barrier, near + planes - 1 + len(turns))

    def send_vol(n):
        (ox, oy, oz), far = VOLUME[n]
        if oz:
            src = pk1.at[1 if oz > 0 else 0]
            dst = ed1.at[0 if oz > 0 else 1, 1 - ox, 1 - oy]
        elif oy == 0:
            own = dx if (ox < 0) != far else 2 * dx - 1
            to = own - dx * ox
            src = r1.at[own, 3 : 3 + dy]
            dst = r1.at[to, 3 : 3 + dy]
        else:
            src_y = 3 if oy < 0 else dy
            dst_y = 0 if oy > 0 else 3 + dy
            to = dx * (1 - ox)
            src = r1.at[dx : 2 * dx, src_y : src_y + 3]
            dst = r1.at[to : to + dx, dst_y : dst_y + 3]
        return copy(src, dst, xs1.at[n], xr1.at[n], at(ox, oy, oz))

    def back(o):
        return there(*(-c for c in o))

    for n, (o, _) in enumerate(VOLUME):
        guarded(there(*o), lambda: send_vol(n).start())

    def take_vol(test):
        for n, (o, far) in enumerate(VOLUME):
            if test(o, far):
                guarded(back(o), lambda: send_vol(n).wait_recv())

    for step in loads[1:]:
        step.wait()
    taps = w_first.shape[0]
    third = taps // 3
    w1t[0:chan, :] = w_first[...].T
    w1t[chan:two, :] = v_first[...].T
    for f, w_ref in enumerate((w_second, v_second)):
        turned = w_ref[...].T
        for kx in range(3):
            w2t[chan * (2 - kx) : chan * (3 - kx), third * f : third * (f + 1)] = turned[:, third * kx : third * (kx + 1)]
    for k in range(27):
        kx, rest = k // 9, k % 9
        w3t[chan * (2 - kx) : chan * (3 - kx), chan * rest : chan * (rest + 1)] = w_second[chan * (26 - k) : chan * (27 - k), :]
    for x in range(dx):
        zero(ej.at[x, 0:3])
        zero(ej.at[x, 3 + dy : 5 + dy])
        zero(eb.at[x, 0:3])
        zero(eb.at[x, 3 + dy : 5 + dy])

    def shift(raw_ref, out_ref, x, y, left, right, j):
        raw = raw_ref[x, y]
        before = left if j == 0 else pltpu.roll(left, 128 - j, 1)
        after = right if j == 127 else pltpu.roll(right, 127 - j, 1)
        out_ref[x, y, 0:chan] = jnp.where(lane == 0, before, pltpu.roll(raw, 1, 1))
        out_ref[x, y, chan:two] = jnp.where(lane == 127, after, pltpu.roll(raw, 127, 1))

    def turn(raw_ref, out_ref, x, y):
        raw = raw_ref[x, y]
        out_ref[x, y, 0:chan] = pltpu.roll(raw, 1, 1)
        out_ref[x, y, chan:two] = pltpu.roll(raw, 127, 1)

    def patch(out_ref, x, y, left, right, j):
        before = left if j == 0 else pltpu.roll(left, 128 - j, 1)
        after = right if j == 127 else pltpu.roll(right, 127 - j, 1)
        out_ref[x, y, 0:chan] = jnp.where(lane == 0, before, out_ref[x, y, 0:chan])
        out_ref[x, y, chan:two] = jnp.where(lane == 127, after, out_ref[x, y, chan:two])

    def slab1(which, lines, turned=False):
        for x in which:
            for y in lines:
                bx, by = x // dx, (y + dy - 3) // dy
                place = (ed1[0, bx, by], ed1[1, bx, by], (x % dx) * dy + (y + dy - 3) % dy)
                if turned:
                    patch(q1, x, y, *place)
                else:
                    shift(r1, q1, x, y, *place)

    def three(raw_ref, out_ref, x, y):
        return [out_ref[x, y, 0:chan], raw_ref[x, y], out_ref[x, y, chan:two]]

    def layer1(x, y, carry):
        halves = []
        for half in range(2):
            pieces = []
            for kx in range(3):
                for ky in range(3):
                    pieces += three(r1, q1, x + kx, y + half + ky)
            halves.append(jnp.concatenate(pieces, axis=0))
        both = jnp.dot(w1t[...], jnp.concatenate(halves, axis=1), preferred_element_type=F32)
        hidden, slope = gelu_pair(both[0:chan])
        gx_cell = ix * dx + x - 1
        gy_cell = iy * dy + y - 2
        inside = jnp.logical_and(
            jnp.logical_and(gx_cell >= 0, gx_cell < nx * dx), jnp.logical_and(gy_cell >= 0, gy_cell < ny * dy)
        )
        keep = inside.astype(F32)
        tangent = (keep * (slope * both[chan:two])).astype(BF16)
        hidden = (keep * hidden).astype(BF16)
        fields = [carry[0:2], carry[2:4]]
        for half in range(2):
            cols = slice(128 * half, 128 * half + 128)
            for f, value in enumerate((tangent, hidden)):
                r2[f, x, y + half] = value[:, cols]
                fields[f] = packed(value[:, cols], x * hy + y + half, fields[f])
            slope_ref[x, y + half] = slope[:, cols]
        return (*fields[0], *fields[1])

    own_y = range(3, 3 + dy)
    halo_y = [*range(3), *range(3 + dy, 6 + dy)]
    inner = (dy - 4) // 2
    for x in range(dx, 2 * dx):
        for y in own_y:
            turn(r1, q1, x, y)
    take_vol(lambda o, far: o[0] == 0 and o[1] == 0)
    slab1(range(dx, 2 * dx), own_y, True)
    take_vol(lambda o, far: o[0] != 0 and o[1] == 0 and not far)
    slab1((dx - 1, 2 * dx), own_y)
    edges = lax.fori_loop(
        0, dx * inner, lambda i, c: layer1(1 + i // inner, 4 + 2 * lax.rem(i, inner), c), (blank,) * 4, unroll=6
    )
    take_vol(lambda o, far: o[1] != 0)
    slab1(range(1, 3 * dx - 1), halo_y)

    def outer(i, c):
        k = lax.rem(i, 4)
        return layer1(1 + i // 4, 2 * lax.rem(k, 2) + dy * (k // 2), c)

    edges = lax.fori_loop(0, dx * 4, outer, edges, unroll=8)
    take_vol(lambda o, far: far)
    slab1((0, 3 * dx - 1), range(dy + 6))
    pairs = hy // 2
    edges = lax.fori_loop(
        0, 2 * pairs, lambda i, c: layer1((hx - 1) * (i // pairs), 2 * lax.rem(i, pairs), c), edges, unroll=10
    )
    pk2[0, 0], pk2[1, 0], pk2[0, 1], pk2[1, 1] = edges

    def send_hid(n, oz):
        return copy(pk2.at[n], ed2.at[1 - n], xs2.at[n], xr2.at[n], at(0, 0, oz))

    for n, oz in enumerate((-1, 1)):
        guarded(there(0, 0, oz), lambda: send_hid(n, oz).start())
    for f in range(2):
        for x in range(hx):
            for y in range(hy):
                turn(r2.at[f], q2.at[f], x, y)
    for n, oz in enumerate((-1, 1)):
        guarded(there(0, 0, -oz), lambda: send_hid(n, oz).wait_recv())

    for f in range(2):
        for x in range(hx):
            for y in range(hy):
                patch(q2.at[f], x, y, ed2[0, f], ed2[1, f], x * hy + y)

    def layer2(pair, carry):
        y = 2 * pair
        out = [None] * dx
        for x in range(hx):
            halves = []
            for half in range(2):
                pieces = []
                for f in range(2):
                    for ky in range(3):
                        pieces += three(r2.at[f], q2.at[f], x, y + half + ky)
                halves.append(jnp.concatenate(pieces, axis=0))
            low, high = max(0, x - 2), min(dx - 1, x)
            left = w2t[chan * (2 - x + low) : chan * (3 - x + high), :]
            product = jnp.dot(left, jnp.concatenate(halves, axis=1), preferred_element_type=F32)
            for to in range(low, high + 1):
                term = product[chan * (to - low) : chan * (to - low + 1)]
                out[to] = term if out[to] is None else out[to] + term
        for x in range(dx):
            for half in range(2):
                gy_cell = iy * dy + y + half - 1
                keep = jnp.logical_and(gy_cell >= 0, gy_cell < ny * dy).astype(F32)
                value = (keep * out[x][:, 128 * half : 128 * half + 128]).astype(BF16)
                r3[x + 1, y + half] = value
                carry = packed(value, x * (dy + 2) + y + half, carry)
        return carry

    cut = 2 * ((dy + 2 + 2) // 4)

    def send_plane(n, ox, late):
        lines = slice(cut, dy + 2) if late else slice(0, cut)
        return copy(
            r3.at[1 if ox < 0 else dx, lines], r3.at[dx + 1 if ox < 0 else 0, lines],
            ps3.at[n, int(late)], pr3.at[n, int(late)], at(ox, 0, 0),
        )

    def send_jv(n):
        ox, oz = SIDES[n]
        return copy(pk3.at[1 if oz > 0 else 0], ed3.at[0 if oz > 0 else 1, 1 - ox], xs3.at[n], xr3.at[n], at(ox, 0, oz))

    edges = lax.fori_loop(0, cut // 2, layer2, (blank, blank), unroll=cut // 2)
    for n, ox in enumerate((-1, 1)):
        guarded(there(ox, 0, 0), lambda: send_plane(n, ox, False).start())
    rest = (dy + 2 - cut) // 2
    pk3[0], pk3[1] = lax.fori_loop(0, rest, lambda i, c: layer2(cut // 2 + i, c), edges, unroll=rest)
    for n, (ox, oz) in enumerate(SIDES):
        guarded(there(ox, 0, oz), lambda: send_jv(n).start())
    for n, ox in enumerate((-1, 1)):
        guarded(there(ox, 0, 0), lambda: send_plane(n, ox, True).start())

    for x in range(dx):
        own = r3[x + 1, 1 : 1 + dy]
        ej[x, 3 : 3 + dy] = own

    def correlate(raw_ref, out_ref, x0, y0, e_ref):
        total = None
        for x in range(dx):
            lhs, rhs = [], []
            for q in range(dy + 2):
                pieces = []
                for kx in range(3):
                    pieces += three(raw_ref, out_ref, x + kx + x0, q + y0)
                lhs.append(jnp.concatenate(pieces, axis=0))
                rhs.append(jnp.concatenate([e_ref[x, q - ky + 3] for ky in range(4)], axis=0))
            product = lax.dot_general(
                jnp.concatenate(lhs, axis=1), jnp.concatenate(rhs, axis=1),
                (((1,), (1,)), ((), ())), preferred_element_type=F32,
            )
            total = product if total is None else total + product
        return total

    lane8 = lax.broadcasted_iota(jnp.int32, (8, 128), 1)

    def put_part(f, value):
        for t in range(nz * wide):
            if t < 27:
                j, s = t // 9, t % 9
                tail = pltpu.roll(value[216 + 8 * s : 224 + 8 * s], 96 - 32 * j, 1)
                part[t, f] = jnp.where(lane8 < 96, value[8 * t : 8 * t + 8], tail)
            else:
                part[t, f] = jnp.zeros((8, 128), F32)

    def send_a(f, n):
        ez, ec = turns[n]
        return copy(part.at[zs[ez] * wide + cs[ec], f], recv_a.at[f, n], sa.at[f], ra.at[f], a_peer(n))

    def send_z(f, d):
        return copy(sum_a.at[f], recv_z.at[f, level], sz.at[f], rz.at[f], z_peer(d))

    def send_g(f, n):
        return copy(fin.at[f], tot.at[me, f], sg.at[f], rg.at[f], a_peer(n))

    def settle(ref, sem):
        pltpu.make_async_copy(ref, ref, sem).wait()

    def start_a(f, value):
        put_part(f, value)
        for n in range(len(turns)):
            send_a(f, n).start()

    def start_z(f):
        settle(recv_a.at[f], ra.at[f])
        total = part[me, f]
        for n in range(len(turns)):
            total = total + recv_a[f, n]
        sum_a[f] = total
        for d in range(1, planes):
            send_z(f, d).start()
        recv_z[f, level] = total

    def start_g(f):
        settle(recv_z.at[f, 1:planes], rz.at[f])
        total = recv_z[f, 0]
        for d in range(1, planes):
            total = total + recv_z[f, d]
        fin[f] = total
        for n in range(len(turns)):
            send_g(f, n).start()
        tot[me, f] = total

    start_a(0, correlate(r2.at[1], q2.at[1], 0, 1, ej))

    def take_jv(own):
        for n, (ox, oz) in enumerate(SIDES):
            if (ox == 0) == own:
                guarded(there(-ox, 0, -oz), lambda: send_jv(n).wait_recv())

    def slab3(which, turned=False):
        for x in which:
            bx = (x + dx - 1) // dx
            for y in range(dy + 2):
                place = (ed3[0, bx], ed3[1, bx], ((x + dx - 1) % dx) * (dy + 2) + y)
                if turned:
                    patch(q3, x, y, *place)
                else:
                    shift(r3, q3, x, y, *place)

    def layer3(x, y):
        halves = []
        for half in range(2):
            pieces = []
            for ky in range(3):
                pieces += three(r3, q3, x, y + half + ky)
            halves.append(jnp.concatenate(pieces, axis=0))
        low, high = max(0, x - 2), min(dx - 1, x)
        left = w3t[chan * (2 - x + low) : chan * (3 - x + high), :]
        product = jnp.dot(left, jnp.concatenate(halves, axis=1), preferred_element_type=F32)
        return {to: product[chan * (to - low) : chan * (to - low + 1)] for to in range(low, high + 1)}

    for x in range(1, dx + 1):
        for y in range(dy + 2):
            turn(r3, q3, x, y)
    take_jv(True)
    slab3(range(1, dx + 1), True)

    def own3(pair, _):
        y = 2 * pair
        parts = [layer3(x, y) for x in range(1, dx + 1)]
        for x in range(dx):
            summed = parts[0][x] + parts[1][x]
            for half in range(2):
                acc3[x, y + half] = summed[:, 128 * half : 128 * half + 128]
        return 0

    lax.fori_loop(0, dy // 2, own3, 0, unroll=4)
    take_jv(False)
    for n, ox in enumerate((-1, 1)):
        for late in (False, True):
            guarded(there(-ox, 0, 0), lambda: send_plane(n, ox, late).wait_recv())
    slab3((0, dx + 1))

    def halo3(pair, _):
        y = 2 * pair
        for x, plane_x in ((0, 0), (dx - 1, dx + 1)):
            term = layer3(plane_x, y)[x]
            for half in range(2):
                cols = slice(128 * half, 128 * half + 128)
                value = slope_ref[x + 1, y + half + 2] * (acc3[x, y + half] + term[:, cols])
                eb[x, y + half + 3] = value.astype(BF16)
        return 0

    lax.fori_loop(0, dy // 2, halo3, 0, unroll=4)

    start_z(0)
    start_a(1, correlate(r1, q1, 1, 2, eb))
    for x in range(dx):
        jv_out[:, x] = jnp.transpose(r3[x + 1, 1 : 1 + dy], (1, 0, 2))
    start_g(0)
    start_z(1)
    start_g(1)
    for f in range(2):
        settle(recv_a.at[f], rg.at[f])

    for n, (o, _) in enumerate(VOLUME):
        guarded(there(*o), lambda: send_vol(n).wait_send())
    for n, oz in enumerate((-1, 1)):
        guarded(there(0, 0, oz), lambda: send_hid(n, oz).wait_send())
    for n, ox in enumerate((-1, 1)):
        for late in (False, True):
            guarded(there(ox, 0, 0), lambda: send_plane(n, ox, late).wait_send())
    for n, (ox, oz) in enumerate(SIDES):
        guarded(there(ox, 0, oz), lambda: send_jv(n).wait_send())
    for f in range(2):
        settle(recv_a.at[f], sa.at[f])
        settle(recv_a.at[f], sg.at[f])
        settle(recv_z.at[f, 1:planes], sz.at[f])


def last_kernel(count_all, factor, tot, jv_in, v_first, v_second, jv, gv_first, gv_second):
    jv[...] = jv_in[...]
    for f, (v_ref, out) in enumerate(((v_second, gv_second), (v_first, gv_first))):
        tile = [tot[t, f] for t in range(27)]
        for kx in range(3):
            for ky in range(3):
                pieces = []
                for u in range(12 * kx, 12 * kx + 12):
                    if u < 27:
                        piece = tile[u] if ky == 0 else pltpu.roll(tile[u], 128 - 32 * ky, 1)
                    else:
                        piece = pltpu.roll(tile[9 * ky + u - 27], 32, 1)
                    pieces.append(piece[:, 0:32])
                k = 3 * kx + ky
                summed = jnp.concatenate(pieces, axis=0)
                base = v_ref[96 * k : 96 * k + 96, :].astype(F32)
                out[k] = factor * (summed / count_all + 0.1 * base)


def body(volume, w_first, w_second, v_first, v_second):
    chan, dx, dy, dz = volume.shape
    nx, ny, nz = lax.axis_size("gx"), lax.axis_size("gy"), lax.axis_size("gz")
    group = 4 * nz
    planes = nx * ny // 4
    count_all = float(dx * dy * dz * nx * ny * nz)
    factor = math.sqrt(27.0 * chan)
    shape = w_first.shape
    flat = [w.reshape(27 * chan, chan) for w in (w_first, w_second, v_first, v_second)]
    vm = pl.BlockSpec(memory_space=pltpu.VMEM)
    far = functools.partial(pltpu.with_memory_space_constraint, memory_space=pltpu.HBM)
    near = functools.partial(pltpu.with_memory_space_constraint, memory_space=pltpu.VMEM)
    dma = pltpu.SemaphoreType.DMA
    tot, jv_made = pl.pallas_call(
        functools.partial(main_kernel, nx, ny, nz, dx, dy),
        out_shape=(
            pltpu.VMEM((group, 2, 8, 128), F32),
            pltpu.VMEM((chan, dx, dy, 128), BF16),
        ),
        in_specs=[pl.BlockSpec(memory_space=pltpu.HBM)] * 5,
        out_specs=(vm, vm),
        scratch_shapes=[
            pltpu.VMEM(volume.shape, BF16),
            *[pltpu.VMEM(flat[0].shape, BF16)] * 4,
            dma((5,)),
            pltpu.VMEM((3 * dx, dy + 6, chan, 128), BF16),
            pltpu.VMEM((3 * dx, dy + 6, 2 * chan, 128), BF16),
            pltpu.VMEM((2, dx + 2, dy + 4, chan, 128), BF16),
            pltpu.VMEM((2, dx + 2, dy + 4, 2 * chan, 128), BF16),
            pltpu.VMEM((dx + 2, dy + 2, chan, 128), BF16),
            pltpu.VMEM((dx + 2, dy + 2, 2 * chan, 128), BF16),
            pltpu.VMEM((dx + 2, dy + 4, chan, 128), F32),
            pltpu.VMEM((dx, dy, chan, 128), F32),
            pltpu.VMEM((dx, dy + 5, chan, 128), BF16),
            pltpu.VMEM((dx, dy + 5, chan, 128), BF16),
            pltpu.VMEM((2 * chan, 27 * chan), BF16),
            pltpu.VMEM((3 * chan, 18 * chan), BF16),
            pltpu.VMEM((3 * chan, 9 * chan), BF16),
            pltpu.VMEM((2, chan, 128), BF16),
            pltpu.VMEM((2, 3, 3, chan, 128), BF16),
            pltpu.VMEM((2, 2, chan, 128), BF16),
            pltpu.VMEM((2, 2, chan, 128), BF16),
            pltpu.VMEM((2, chan, 128), BF16),
            pltpu.VMEM((2, 3, chan, 128), BF16),
            pltpu.VMEM((group, 2, 8, 128), F32),
            pltpu.VMEM((2, group - 1, 8, 128), F32),
            pltpu.VMEM((2, 8, 128), F32),
            pltpu.VMEM((2, planes, 8, 128), F32),
            pltpu.VMEM((2, 8, 128), F32),
            dma((len(VOLUME),)), dma((len(VOLUME),)),
            dma((2,)), dma((2,)),
            dma((6,)), dma((6,)),
            dma((2, 2)), dma((2, 2)),
            *[dma((2,))] * 6,
        ],
        compiler_params=pltpu.CompilerParams(collective_id=0, has_side_effects=True, vmem_limit_bytes=40 << 20),
        cost_estimate=pl.CostEstimate(flops=2000000000, bytes_accessed=2000000, transcendentals=400000),
    )(*[far(array) for array in (volume, *flat)])
    jv, gv_first, gv_second = pl.pallas_call(
        functools.partial(last_kernel, count_all, factor),
        out_shape=(
            jax.ShapeDtypeStruct(volume.shape, BF16),
            jax.ShapeDtypeStruct((9, 3 * chan, chan), F32),
            jax.ShapeDtypeStruct((9, 3 * chan, chan), F32),
        ),
        in_specs=[vm] * 4,
        out_specs=(vm, vm, vm),
        compiler_params=pltpu.CompilerParams(vmem_limit_bytes=8 << 20),
    )(near(tot), near(jv_made), flat[2], flat[3])
    return (jv, gv_first.reshape(shape), gv_second.reshape(shape))


def solution(mesh):
    in_specs = (P(None, "gx", "gy", "gz"), P(), P(), P(), P())
    out_specs = (P(None, "gx", "gy", "gz"), P(), P())
    return jax.shard_map(body, mesh=mesh, in_specs=in_specs, out_specs=out_specs, check_vma=False)
```

```python
import functools
import itertools
import math

import jax
import jax.numpy as jnp
from jax import lax
from jax.experimental import pallas as pl
from jax.experimental.pallas import tpu as pltpu
from jax.sharding import PartitionSpec as P

MESH = pl.DeviceIdType.MESH
BF16 = jnp.bfloat16
F32 = jnp.float32
OFFSETS = [o for o in itertools.product((-1, 0, 1), repeat=3) if o != (0, 0, 0)]
VOLUME = [(o, False) for o in OFFSETS if o[1] != 0 and o[2] == 0]
VOLUME += [(o, False) for o in OFFSETS if o[1] != 0 and o[2] != 0]
VOLUME += [((ox, 0, 0), False) for ox in (-1, 1)]
VOLUME += [((ox, 0, oz), False) for ox in (0, -1, 1) for oz in (-1, 1)]
VOLUME += [((ox, 0, 0), True) for ox in (-1, 1)]
SIDES = [(ox, oz) for ox in (-1, 0, 1) for oz in (-1, 1)]


def gelu_pair(pre):
    square = pre * pre
    hyper = jnp.tanh(0.7978845608 * (pre + 0.044715 * square * pre))
    half = 0.5 * (1.0 + hyper)
    hidden = pre * half
    slope = half + (0.5 * pre) * (1.0 - hyper * hyper) * (0.7978845608 * (1.0 + 0.134145 * square))
    return (hidden, slope)


def main_kernel(
    nx, ny, nz, dx, dy,
    vol_in, w_first_in, w_second_in, v_first_in, v_second_in,
    tot, jv_out,
    vol, w_first, w_second, v_first, v_second, load, r1, q1, r2, q2, r3, q3, slope_ref, acc3, ej, eb, w1t, w2t, w3t,
    pk1, ed1, pk2, ed2, pk3, ed3,
    part, recv_a, sum_a, recv_z, fin,
    xs1, xr1, xs2, xr2, xs3, xr3, ps3, pr3,
    sa, ra, sz, rz, sg, rg,
):
    ix, iy, iz = lax.axis_index("gx"), lax.axis_index("gy"), lax.axis_index("gz")
    me = iy * nx + ix
    chan = vol.shape[0]
    two = 2 * chan
    hx, hy = dx + 2, dy + 4
    lane = lax.broadcasted_iota(jnp.int32, (chan, 128), 1)

    def there(ox, oy, oz):
        ok = None
        for offset, index, count in ((ox, ix, nx), (oy, iy, ny), (oz, iz, nz)):
            if offset:
                one = index < count - 1 if offset > 0 else index > 0
                ok = one if ok is None else jnp.logical_and(ok, one)
        return ok

    def at(ox, oy, oz):
        return {"gx": ix + ox, "gy": iy + oy, "gz": iz + oz}

    wide = 4
    high = ny // wide
    planes = high * nx
    col, row = lax.rem(iy, wide), iy // wide
    level = row * nx + ix
    rings = nz // 2
    core, ring = lax.rem(iz, 2), iz // 2
    gs = [lax.rem(ring + d, rings) for d in range(rings)]
    cs = [lax.rem(col + d, wide) for d in range(wide)]
    turns = [(eg, ec) for eg in range(rings) for ec in range(wide)]
    me = ring * wide + col

    def a_peer(n, side):
        eg, ec = turns[n]
        return {"gx": ix, "gy": row * wide + cs[ec], "gz": 2 * gs[eg] + side}

    def z_peer(d):
        other = lax.rem(level + d, planes)
        return {"gx": lax.rem(other, nx), "gy": (other // nx) * wide + col, "gz": iz}

    def copy(src, dst, send, recv, peer):
        return pltpu.make_async_remote_copy(src, dst, send, recv, device_id=peer, device_id_type=MESH)

    def guarded(cond, action):
        @pl.when(cond)
        def _():
            action()

    loads = [
        pltpu.make_async_copy(src, dst, load.at[n])
        for n, (src, dst) in enumerate(
            ((vol_in, vol), (w_first_in, w_first), (w_second_in, w_second), (v_first_in, v_first), (v_second_in, v_second))
        )
    ]
    for step in loads:
        step.start()
    barrier = pltpu.get_barrier_semaphore()

    def greet(peer):
        pl.semaphore_signal(barrier, inc=1, device_id=peer, device_id_type=MESH)

    for d in range(1, planes):
        greet(z_peer(d))
    for n in range(1, len(turns)):
        greet(a_peer(n, 0))
        greet(a_peer(n, 1))
    greet(a_peer(0, 1 - core))
    for o in OFFSETS:
        guarded(there(*o), lambda: greet(at(*o)))

    def zero(ref):
        ref[...] = jnp.zeros(ref.shape, ref.dtype)

    loads[0].wait()
    for x in range(dx):
        r1[dx + x, 3 : 3 + dy] = jnp.transpose(vol[:, x], (1, 0, 2))

    def packed(raw, j, pair):
        first = jnp.where(lane == j, jnp.broadcast_to(raw[:, 0:1], raw.shape), pair[0])
        last = jnp.where(lane == j, jnp.broadcast_to(raw[:, 127:128], raw.shape), pair[1])
        return first, last

    blank = jnp.zeros((chan, 128), BF16)
    half_lane = lane[0:16]
    edges = [blank[0:16], blank[0:16]]
    for x in range(dx):
        for y in range(dy):
            raw = r1[dx + x, 3 + y]
            for part_of in range(2):
                piece = raw[16 * part_of : 16 * part_of + 16]
                here = half_lane == x * dy + y + 64 * part_of
                for n, column in enumerate((piece[:, 0:1], piece[:, 127:128])):
                    edges[n] = jnp.where(here, jnp.broadcast_to(column, piece.shape), edges[n])
    pk1[0], pk1[1] = edges

    @pl.when(ix == 0)
    def _():
        zero(r1.at[0:dx])
        zero(ed1.at[:, 0])
        zero(r3.at[0])
        zero(ed3.at[:, 0])

    @pl.when(ix == nx - 1)
    def _():
        zero(r1.at[2 * dx : 3 * dx])
        zero(ed1.at[:, 2])
        zero(r3.at[dx + 1])
        zero(ed3.at[:, 2])

    @pl.when(iy == 0)
    def _():
        zero(r1.at[:, 0:3])
        zero(ed1.at[:, :, 0])

    @pl.when(iy == ny - 1)
    def _():
        zero(r1.at[:, 3 + dy : 6 + dy])
        zero(ed1.at[:, :, 2])

    @pl.when(iz == 0)
    def _():
        zero(ed1.at[0])
        zero(ed2.at[0])
        zero(ed3.at[0])

    @pl.when(iz == nz - 1)
    def _():
        zero(ed1.at[1])
        zero(ed2.at[1])
        zero(ed3.at[1])

    def span(index, count):
        return 3 - (index == 0).astype(jnp.int32) - (index == count - 1).astype(jnp.int32)

    near = span(ix, nx) * span(iy, ny) * span(iz, nz) - 1
    pl.semaphore_wait(barrier, near + planes - 1 + 2 * len(turns) - 1)

    def send_vol(n):
        (ox, oy, oz), far = VOLUME[n]
        if oz:
            src = pk1.at[1 if oz > 0 else 0]
            dst = ed1.at[0 if oz > 0 else 1, 1 - ox, 1 - oy]
        elif oy == 0:
            own = dx if (ox < 0) != far else 2 * dx - 1
            to = own - dx * ox
            src = r1.at[own, 3 : 3 + dy]
            dst = r1.at[to, 3 : 3 + dy]
        else:
            src_y = 3 if oy < 0 else dy
            dst_y = 0 if oy > 0 else 3 + dy
            to = dx * (1 - ox)
            src = r1.at[dx : 2 * dx, src_y : src_y + 3]
            dst = r1.at[to : to + dx, dst_y : dst_y + 3]
        return copy(src, dst, xs1.at[n], xr1.at[n], at(ox, oy, oz))

    def back(o):
        return there(*(-c for c in o))

    for n, (o, _) in enumerate(VOLUME):
        guarded(there(*o), lambda: send_vol(n).start())

    def take_vol(test):
        for n, (o, far) in enumerate(VOLUME):
            if test(o, far):
                guarded(back(o), lambda: send_vol(n).wait_recv())

    for step in loads[1:]:
        step.wait()
    taps = w_first.shape[0]
    third = taps // 3
    w1t[0:chan, :] = w_first[...].T
    w1t[chan:two, :] = v_first[...].T
    for f, w_ref in enumerate((w_second, v_second)):
        turned = w_ref[...].T
        for kx in range(3):
            w2t[chan * (2 - kx) : chan * (3 - kx), third * f : third * (f + 1)] = turned[:, third * kx : third * (kx + 1)]
    for k in range(27):
        kx, rest = k // 9, k % 9
        w3t[chan * (2 - kx) : chan * (3 - kx), chan * rest : chan * (rest + 1)] = w_second[chan * (26 - k) : chan * (27 - k), :]
    for x in range(dx):
        zero(ej.at[x, 0:3])
        zero(ej.at[x, 3 + dy : 5 + dy])
        zero(eb.at[x, 0:3])
        zero(eb.at[x, 3 + dy : 5 + dy])

    def shift(raw_ref, out_ref, x, y, left, right, j):
        raw = raw_ref[x, y]
        before = left if not j else pltpu.roll(left, 128 - j, 1)
        after = right if j is None else pltpu.roll(right, 127 - j, 1)
        out_ref[x, y, 0:chan] = jnp.where(lane == 0, before, pltpu.roll(raw, 1, 1))
        out_ref[x, y, chan:two] = jnp.where(lane == 127, after, pltpu.roll(raw, 127, 1))

    def turn(raw_ref, out_ref, x, y):
        raw = raw_ref[x, y]
        out_ref[x, y, 0:chan] = pltpu.roll(raw, 1, 1)
        out_ref[x, y, chan:two] = pltpu.roll(raw, 127, 1)

    def patch(out_ref, x, y, left, right, j):
        before = left if not j else pltpu.roll(left, 128 - j, 1)
        after = right if j is None else pltpu.roll(right, 127 - j, 1)
        out_ref[x, y, 0:chan] = jnp.where(lane == 0, before, out_ref[x, y, 0:chan])
        out_ref[x, y, chan:two] = jnp.where(lane == 127, after, out_ref[x, y, chan:two])

    def spread(tile, j, to):
        shifts = [(to - j - 64 * part_of) % 128 for part_of in range(2)]
        return jnp.concatenate([pltpu.roll(tile, k, 1) if k else tile for k in shifts], axis=0)

    def slab1(which, lines, turned=False):
        for x in which:
            for y in lines:
                bx, by = x // dx, (y + dy - 3) // dy
                j = (x % dx) * dy + (y + dy - 3) % dy
                place = (spread(ed1[0, bx, by], j, 0), spread(ed1[1, bx, by], j, 127), None)
                if turned:
                    patch(q1, x, y, *place)
                else:
                    shift(r1, q1, x, y, *place)

    def three(raw_ref, out_ref, x, y):
        return [out_ref[x, y, 0:chan], raw_ref[x, y], out_ref[x, y, chan:two]]

    def layer1(x, y, carry):
        halves = []
        for half in range(2):
            pieces = []
            for kx in range(3):
                for ky in range(3):
                    pieces += three(r1, q1, x + kx, y + half + ky)
            halves.append(jnp.concatenate(pieces, axis=0))
        both = jnp.dot(w1t[...], jnp.concatenate(halves, axis=1), preferred_element_type=F32)
        hidden, slope = gelu_pair(both[0:chan])
        gx_cell = ix * dx + x - 1
        gy_cell = iy * dy + y - 2
        inside = jnp.logical_and(
            jnp.logical_and(gx_cell >= 0, gx_cell < nx * dx), jnp.logical_and(gy_cell >= 0, gy_cell < ny * dy)
        )
        keep = inside.astype(F32)
        tangent = (keep * (slope * both[chan:two])).astype(BF16)
        hidden = (keep * hidden).astype(BF16)
        fields = [carry[0:2], carry[2:4]]
        for half in range(2):
            cols = slice(128 * half, 128 * half + 128)
            for f, value in enumerate((tangent, hidden)):
                r2[f, x, y + half] = value[:, cols]
                fields[f] = packed(value[:, cols], x * hy + y + half, fields[f])
            slope_ref[x, y + half] = slope[:, cols]
        return (*fields[0], *fields[1])

    own_y = range(3, 3 + dy)
    halo_y = [*range(3), *range(3 + dy, 6 + dy)]
    inner = (dy - 4) // 2
    for x in range(dx, 2 * dx):
        for y in own_y:
            turn(r1, q1, x, y)
    take_vol(lambda o, far: o[0] == 0 and o[1] == 0)
    slab1(range(dx, 2 * dx), own_y, True)
    take_vol(lambda o, far: o[0] != 0 and o[1] == 0 and not far)
    slab1((dx - 1, 2 * dx), own_y)
    edges = lax.fori_loop(
        0, dx * inner, lambda i, c: layer1(1 + i // inner, 4 + 2 * lax.rem(i, inner), c), (blank,) * 4, unroll=6
    )
    take_vol(lambda o, far: o[1] != 0)
    slab1(range(1, 3 * dx - 1), halo_y)

    def outer(i, c):
        k = lax.rem(i, 4)
        return layer1(1 + i // 4, 2 * lax.rem(k, 2) + dy * (k // 2), c)

    edges = lax.fori_loop(0, dx * 4, outer, edges, unroll=8)
    take_vol(lambda o, far: far)
    slab1((0, 3 * dx - 1), range(dy + 6))
    pairs = hy // 2
    edges = lax.fori_loop(
        0, 2 * pairs, lambda i, c: layer1((hx - 1) * (i // pairs), 2 * lax.rem(i, pairs), c), edges, unroll=10
    )
    pk2[0, 0], pk2[1, 0], pk2[0, 1], pk2[1, 1] = edges

    def send_hid(n, oz):
        return copy(pk2.at[n], ed2.at[1 - n], xs2.at[n], xr2.at[n], at(0, 0, oz))

    for n, oz in enumerate((-1, 1)):
        guarded(there(0, 0, oz), lambda: send_hid(n, oz).start())
    for f in range(2):
        for x in range(hx):
            for y in range(hy):
                turn(r2.at[f], q2.at[f], x, y)
    for n, oz in enumerate((-1, 1)):
        guarded(there(0, 0, -oz), lambda: send_hid(n, oz).wait_recv())

    for f in range(2):
        for x in range(hx):
            for y in range(hy):
                patch(q2.at[f], x, y, ed2[0, f], ed2[1, f], x * hy + y)

    def layer2(pair, carry):
        y = 2 * pair
        out = [None] * dx
        for x in range(hx):
            halves = []
            for half in range(2):
                pieces = []
                for f in range(2):
                    for ky in range(3):
                        pieces += three(r2.at[f], q2.at[f], x, y + half + ky)
                halves.append(jnp.concatenate(pieces, axis=0))
            low, high = max(0, x - 2), min(dx - 1, x)
            left = w2t[chan * (2 - x + low) : chan * (3 - x + high), :]
            product = jnp.dot(left, jnp.concatenate(halves, axis=1), preferred_element_type=F32)
            for to in range(low, high + 1):
                term = product[chan * (to - low) : chan * (to - low + 1)]
                out[to] = term if out[to] is None else out[to] + term
        for x in range(dx):
            for half in range(2):
                gy_cell = iy * dy + y + half - 1
                keep = jnp.logical_and(gy_cell >= 0, gy_cell < ny * dy).astype(F32)
                value = (keep * out[x][:, 128 * half : 128 * half + 128]).astype(BF16)
                r3[x + 1, y + half] = value
                carry = packed(value, x * (dy + 2) + y + half, carry)
        return carry

    cut = 2 * ((dy + 2 + 2) // 4)

    def send_plane(n, ox, late):
        lines = slice(cut, dy + 2) if late else slice(0, cut)
        return copy(
            r3.at[1 if ox < 0 else dx, lines], r3.at[dx + 1 if ox < 0 else 0, lines],
            ps3.at[n, int(late)], pr3.at[n, int(late)], at(ox, 0, 0),
        )

    def send_jv(n):
        ox, oz = SIDES[n]
        return copy(pk3.at[1 if oz > 0 else 0], ed3.at[0 if oz > 0 else 1, 1 - ox], xs3.at[n], xr3.at[n], at(ox, 0, oz))

    edges = lax.fori_loop(0, cut // 2, layer2, (blank, blank), unroll=cut // 2)
    for n, ox in enumerate((-1, 1)):
        guarded(there(ox, 0, 0), lambda: send_plane(n, ox, False).start())
    rest = (dy + 2 - cut) // 2
    pk3[0], pk3[1] = lax.fori_loop(0, rest, lambda i, c: layer2(cut // 2 + i, c), edges, unroll=rest)
    for n, (ox, oz) in enumerate(SIDES):
        guarded(there(ox, 0, oz), lambda: send_jv(n).start())
    for n, ox in enumerate((-1, 1)):
        guarded(there(ox, 0, 0), lambda: send_plane(n, ox, True).start())

    for x in range(dx):
        own = r3[x + 1, 1 : 1 + dy]
        ej[x, 3 : 3 + dy] = own

    def correlate(raw_ref, out_ref, x0, y0, e_ref):
        total = None
        for x in range(dx):
            lhs, rhs = [], []
            for q in range(dy + 2):
                pieces = []
                for kx in range(3):
                    pieces += three(raw_ref, out_ref, x + kx + x0, q + y0)
                lhs.append(jnp.concatenate(pieces, axis=0))
                rhs.append(jnp.concatenate([e_ref[x, q - ky + 3] for ky in range(4)], axis=0))
            product = lax.dot_general(
                jnp.concatenate(lhs, axis=1), jnp.concatenate(rhs, axis=1),
                (((1,), (1,)), ((), ())), preferred_element_type=F32,
            )
            total = product if total is None else total + product
        return total

    lane8 = lax.broadcasted_iota(jnp.int32, (8, 128), 1)

    def put_part(f, value):
        for t in range(2 * len(turns)):
            if t < 27:
                j, s = t // 9, t % 9
                tail = pltpu.roll(value[216 + 8 * s : 224 + 8 * s], 96 - 32 * j, 1)
                part[t // 2, f, t % 2] = jnp.where(lane8 < 96, value[8 * t : 8 * t + 8], tail)
            else:
                part[t // 2, f, t % 2] = jnp.zeros((8, 128), F32)

    def send_a(f, n):
        eg, ec = turns[n]
        return copy(
            part.at[gs[eg] * wide + cs[ec], f], recv_a.at[f, core * len(turns) + n], sa.at[f], ra.at[f], a_peer(n, 1)
        )

    def send_z(f, d):
        return copy(sum_a.at[f], recv_z.at[f, level], sz.at[f], rz.at[f], z_peer(d))

    def send_g(f, n, side):
        return copy(fin.at[f], tot.at[me, f], sg.at[f], rg.at[f], a_peer(n, side))

    def settle(ref, sem):
        pltpu.make_async_copy(ref, ref, sem).wait()

    count = len(turns)

    def start_a(f, value):
        put_part(f, value)
        for n in range(1, count):
            send_a(f, n).start()

        @pl.when(core == 0)
        def _():
            send_a(f, 0).start()

        @pl.when(core == 1)
        def _():
            recv_a[f, count] = part[me, f]

    def start_z(f):
        @pl.when(core == 1)
        def _():
            settle(recv_a.at[f, 1 : 2 * count], ra.at[f])
            total = recv_a[f, 0]
            for n in range(1, 2 * count):
                total = total + recv_a[f, n]
            sum_a[f] = total
            for d in range(1, planes):
                send_z(f, d).start()
            recv_z[f, level] = total

    def start_g(f):
        @pl.when(core == 1)
        def _():
            settle(recv_z.at[f, 1:planes], rz.at[f])
            total = recv_z[f, 0]
            for d in range(1, planes):
                total = total + recv_z[f, d]
            fin[f] = total
            for n in range(1, count):
                send_g(f, n, 0).start()
                send_g(f, n, 1).start()
            send_g(f, 0, 0).start()
            tot[me, f] = total

    def end_g(f):
        @pl.when(core == 1)
        def _():
            settle(recv_a.at[f, 1:count], rg.at[f])

        @pl.when(core == 0)
        def _():
            settle(recv_a.at[f, 0:count], rg.at[f])

    def leave(f):
        @pl.when(core == 1)
        def _():
            settle(recv_a.at[f, 1:count], sa.at[f])
            settle(recv_z.at[f, 1:planes], sz.at[f])
            settle(recv_a.at[f, 1 : 2 * count], sg.at[f])

        @pl.when(core == 0)
        def _():
            settle(recv_a.at[f, 0:count], sa.at[f])

    start_a(0, correlate(r2.at[1], q2.at[1], 0, 1, ej))

    def take_jv(own):
        for n, (ox, oz) in enumerate(SIDES):
            if (ox == 0) == own:
                guarded(there(-ox, 0, -oz), lambda: send_jv(n).wait_recv())

    def slab3(which, turned=False):
        for x in which:
            bx = (x + dx - 1) // dx
            for y in range(dy + 2):
                place = (ed3[0, bx], ed3[1, bx], ((x + dx - 1) % dx) * (dy + 2) + y)
                if turned:
                    patch(q3, x, y, *place)
                else:
                    shift(r3, q3, x, y, *place)

    def layer3(x, y):
        halves = []
        for half in range(2):
            pieces = []
            for ky in range(3):
                pieces += three(r3, q3, x, y + half + ky)
            halves.append(jnp.concatenate(pieces, axis=0))
        low, high = max(0, x - 2), min(dx - 1, x)
        left = w3t[chan * (2 - x + low) : chan * (3 - x + high), :]
        product = jnp.dot(left, jnp.concatenate(halves, axis=1), preferred_element_type=F32)
        return {to: product[chan * (to - low) : chan * (to - low + 1)] for to in range(low, high + 1)}

    for x in range(1, dx + 1):
        for y in range(dy + 2):
            turn(r3, q3, x, y)
    take_jv(True)
    slab3(range(1, dx + 1), True)

    def own3(pair, _):
        y = 2 * pair
        parts = [layer3(x, y) for x in range(1, dx + 1)]
        for x in range(dx):
            summed = parts[0][x] + parts[1][x]
            for half in range(2):
                acc3[x, y + half] = summed[:, 128 * half : 128 * half + 128]
        return 0

    lax.fori_loop(0, dy // 2, own3, 0, unroll=4)
    take_jv(False)
    for n, ox in enumerate((-1, 1)):
        for late in (False, True):
            guarded(there(-ox, 0, 0), lambda: send_plane(n, ox, late).wait_recv())
    slab3((0, dx + 1))

    def halo3(pair, _):
        y = 2 * pair
        for x, plane_x in ((0, 0), (dx - 1, dx + 1)):
            term = layer3(plane_x, y)[x]
            for half in range(2):
                cols = slice(128 * half, 128 * half + 128)
                value = slope_ref[x + 1, y + half + 2] * (acc3[x, y + half] + term[:, cols])
                eb[x, y + half + 3] = value.astype(BF16)
        return 0

    lax.fori_loop(0, dy // 2, halo3, 0, unroll=4)

    start_a(1, correlate(r1, q1, 1, 2, eb))
    start_z(0)
    for x in range(dx):
        jv_out[:, x] = jnp.transpose(r3[x + 1, 1 : 1 + dy], (1, 0, 2))
    start_g(0)
    start_z(1)
    start_g(1)
    for f in range(2):
        end_g(f)

    for n, (o, _) in enumerate(VOLUME):
        guarded(there(*o), lambda: send_vol(n).wait_send())
    for n, oz in enumerate((-1, 1)):
        guarded(there(0, 0, oz), lambda: send_hid(n, oz).wait_send())
    for n, ox in enumerate((-1, 1)):
        for late in (False, True):
            guarded(there(ox, 0, 0), lambda: send_plane(n, ox, late).wait_send())
    for n, (ox, oz) in enumerate(SIDES):
        guarded(there(ox, 0, oz), lambda: send_jv(n).wait_send())
    for f in range(2):
        leave(f)


def last_kernel(count_all, factor, tot, jv_in, v_first, v_second, jv, gv_first, gv_second):
    jv[...] = jv_in[...]
    for f, (v_ref, out) in enumerate(((v_second, gv_second), (v_first, gv_first))):
        tile = [tot[t // 2, f, t % 2] for t in range(27)]
        for kx in range(3):
            for ky in range(3):
                pieces = []
                for u in range(12 * kx, 12 * kx + 12):
                    if u < 27:
                        piece = tile[u] if ky == 0 else pltpu.roll(tile[u], 128 - 32 * ky, 1)
                    else:
                        piece = pltpu.roll(tile[9 * ky + u - 27], 32, 1)
                    pieces.append(piece[:, 0:32])
                k = 3 * kx + ky
                summed = jnp.concatenate(pieces, axis=0)
                base = v_ref[96 * k : 96 * k + 96, :].astype(F32)
                out[k] = factor * (summed / count_all + 0.1 * base)


def body(volume, w_first, w_second, v_first, v_second):
    chan, dx, dy, dz = volume.shape
    nx, ny, nz = lax.axis_size("gx"), lax.axis_size("gy"), lax.axis_size("gz")
    group = 2 * nz
    planes = nx * ny // 4
    count_all = float(dx * dy * dz * nx * ny * nz)
    factor = math.sqrt(27.0 * chan)
    shape = w_first.shape
    flat = [w.reshape(27 * chan, chan) for w in (w_first, w_second, v_first, v_second)]
    vm = pl.BlockSpec(memory_space=pltpu.VMEM)
    far = functools.partial(pltpu.with_memory_space_constraint, memory_space=pltpu.HBM)
    near = functools.partial(pltpu.with_memory_space_constraint, memory_space=pltpu.VMEM)
    dma = pltpu.SemaphoreType.DMA
    tot, jv_made = pl.pallas_call(
        functools.partial(main_kernel, nx, ny, nz, dx, dy),
        out_shape=(
            pltpu.VMEM((group, 2, 2, 8, 128), F32),
            pltpu.VMEM((chan, dx, dy, 128), BF16),
        ),
        in_specs=[pl.BlockSpec(memory_space=pltpu.HBM)] * 5,
        out_specs=(vm, vm),
        scratch_shapes=[
            pltpu.VMEM(volume.shape, BF16),
            *[pltpu.VMEM(flat[0].shape, BF16)] * 4,
            dma((5,)),
            pltpu.VMEM((3 * dx, dy + 6, chan, 128), BF16),
            pltpu.VMEM((3 * dx, dy + 6, 2 * chan, 128), BF16),
            pltpu.VMEM((2, dx + 2, dy + 4, chan, 128), BF16),
            pltpu.VMEM((2, dx + 2, dy + 4, 2 * chan, 128), BF16),
            pltpu.VMEM((dx + 2, dy + 2, chan, 128), BF16),
            pltpu.VMEM((dx + 2, dy + 2, 2 * chan, 128), BF16),
            pltpu.VMEM((dx + 2, dy + 4, chan, 128), F32),
            pltpu.VMEM((dx, dy, chan, 128), F32),
            pltpu.VMEM((dx, dy + 5, chan, 128), BF16),
            pltpu.VMEM((dx, dy + 5, chan, 128), BF16),
            pltpu.VMEM((2 * chan, 27 * chan), BF16),
            pltpu.VMEM((3 * chan, 18 * chan), BF16),
            pltpu.VMEM((3 * chan, 9 * chan), BF16),
            pltpu.VMEM((2, 16, 128), BF16),
            pltpu.VMEM((2, 3, 3, 16, 128), BF16),
            pltpu.VMEM((2, 2, chan, 128), BF16),
            pltpu.VMEM((2, 2, chan, 128), BF16),
            pltpu.VMEM((2, chan, 128), BF16),
            pltpu.VMEM((2, 3, chan, 128), BF16),
            pltpu.VMEM((group, 2, 2, 8, 128), F32),
            pltpu.VMEM((2, 2 * group, 2, 8, 128), F32),
            pltpu.VMEM((2, 2, 8, 128), F32),
            pltpu.VMEM((2, planes, 2, 8, 128), F32),
            pltpu.VMEM((2, 2, 8, 128), F32),
            dma((len(VOLUME),)), dma((len(VOLUME),)),
            dma((2,)), dma((2,)),
            dma((6,)), dma((6,)),
            dma((2, 2)), dma((2, 2)),
            *[dma((2,))] * 6,
        ],
        compiler_params=pltpu.CompilerParams(collective_id=0, has_side_effects=True, vmem_limit_bytes=40 << 20),
        cost_estimate=pl.CostEstimate(flops=2000000000, bytes_accessed=2000000, transcendentals=400000),
    )(*[far(array) for array in (volume, *flat)])
    jv, gv_first, gv_second = pl.pallas_call(
        functools.partial(last_kernel, count_all, factor),
        out_shape=(
            jax.ShapeDtypeStruct(volume.shape, BF16),
            jax.ShapeDtypeStruct((9, 3 * chan, chan), F32),
            jax.ShapeDtypeStruct((9, 3 * chan, chan), F32),
        ),
        in_specs=[vm] * 4,
        out_specs=(vm, vm, vm),
        compiler_params=pltpu.CompilerParams(vmem_limit_bytes=8 << 20),
    )(near(tot), near(jv_made), flat[2], flat[3])
    return (jv, gv_first.reshape(shape), gv_second.reshape(shape))


def solution(mesh):
    in_specs = (P(None, "gx", "gy", "gz"), P(), P(), P(), P())
    out_specs = (P(None, "gx", "gy", "gz"), P(), P())
    return jax.shard_map(body, mesh=mesh, in_specs=in_specs, out_specs=out_specs, check_vma=False)
```

```python
import functools
import itertools
import math

import jax
import jax.numpy as jnp
from jax import lax
from jax.experimental import pallas as pl
from jax.experimental.pallas import tpu as pltpu
from jax.sharding import PartitionSpec as P

MESH = pl.DeviceIdType.MESH
BF16 = jnp.bfloat16
F32 = jnp.float32
OFFSETS = [o for o in itertools.product((-1, 0, 1), repeat=3) if o != (0, 0, 0)]
VOLUME = []
VOLUME += [(o, False) for o in OFFSETS if o[1] != 0 and o[2] != 0]
VOLUME += [(o, False) for o in OFFSETS if o[1] != 0 and o[0] == 0 and o[2] == 0]
VOLUME += [(o, False) for o in OFFSETS if o[1] != 0 and o[0] != 0 and o[2] == 0]
VOLUME += [((ox, 0, 0), False) for ox in (-1, 1)]
VOLUME += [((ox, 0, oz), False) for ox in (0, -1, 1) for oz in (-1, 1)]
VOLUME += [((ox, 0, 0), True) for ox in (-1, 1)]
SIDES = [(ox, oz) for ox in (-1, 0, 1) for oz in (-1, 1)]


def gelu_pair(pre):
    square = pre * pre
    hyper = jnp.tanh(0.7978845608 * (pre + 0.044715 * square * pre))
    half = 0.5 * (1.0 + hyper)
    hidden = pre * half
    slope = half + (0.5 * pre) * (1.0 - hyper * hyper) * (0.7978845608 * (1.0 + 0.134145 * square))
    return (hidden, slope)


def main_kernel(
    nx, ny, nz, dx, dy,
    vol_in, w_first_in, w_second_in, v_first_in, v_second_in,
    tot, jv_out,
    vol, w_first, w_second, v_first, v_second, load, r1, q1, r2, q2, r3, q3, slope_ref, acc3, ej, eb, w1t, w2t, w3t,
    pk1, ed1, pk2, ed2, pk3, ed3,
    part, recv_a, sum_a, recv_z, fin,
    xs1, xr1, xs2, xr2, xs3, xr3, ps3, pr3,
    sa, ra, sz, rz, sg, rg,
):
    ix, iy, iz = lax.axis_index("gx"), lax.axis_index("gy"), lax.axis_index("gz")
    me = iy * nx + ix
    chan = vol.shape[0]
    two = 2 * chan
    hx, hy = dx + 2, dy + 4
    lane = lax.broadcasted_iota(jnp.int32, (chan, 128), 1)

    def there(ox, oy, oz):
        ok = None
        for offset, index, count in ((ox, ix, nx), (oy, iy, ny), (oz, iz, nz)):
            if offset:
                one = index < count - 1 if offset > 0 else index > 0
                ok = one if ok is None else jnp.logical_and(ok, one)
        return ok

    def at(ox, oy, oz):
        return {"gx": ix + ox, "gy": iy + oy, "gz": iz + oz}

    wide = 4
    high = ny // wide
    planes = high * nx
    col, row = lax.rem(iy, wide), iy // wide
    level = row * nx + ix
    rings = nz // 2
    core, ring = lax.rem(iz, 2), iz // 2
    gs = [lax.rem(ring + d, rings) for d in range(rings)]
    cs = [lax.rem(col + d, wide) for d in range(wide)]
    turns = sorted(
        ((eg, ec) for eg in range(rings) for ec in range(wide)),
        key=lambda t: (t != (0, 0), -min(t[0], rings - t[0]) - min(t[1], wide - t[1])),
    )
    steps = sorted(range(1, planes), key=lambda d: -min(d, planes - d))
    me = ring * wide + col

    def a_peer(n, side):
        eg, ec = turns[n]
        return {"gx": ix, "gy": row * wide + cs[ec], "gz": 2 * gs[eg] + side}

    def z_peer(d):
        other = lax.rem(level + d, planes)
        return {"gx": lax.rem(other, nx), "gy": (other // nx) * wide + col, "gz": iz}

    def copy(src, dst, send, recv, peer):
        return pltpu.make_async_remote_copy(src, dst, send, recv, device_id=peer, device_id_type=MESH)

    def guarded(cond, action):
        @pl.when(cond)
        def _():
            action()

    loads = [
        pltpu.make_async_copy(src, dst, load.at[n])
        for n, (src, dst) in enumerate(
            ((vol_in, vol), (w_first_in, w_first), (w_second_in, w_second), (v_first_in, v_first), (v_second_in, v_second))
        )
    ]
    for step in loads:
        step.start()
    barrier = pltpu.get_barrier_semaphore()

    def greet(peer):
        pl.semaphore_signal(barrier, inc=1, device_id=peer, device_id_type=MESH)

    @pl.when(core == 1)
    def _():
        for d in range(1, planes):
            greet(z_peer(d))
        for n in range(1, len(turns)):
            greet(a_peer(n, 0))

    for n in range(1, len(turns)):
        greet(a_peer(n, 1))
    greet(a_peer(0, 1 - core))
    for o in OFFSETS:
        guarded(there(*o), lambda: greet(at(*o)))

    def zero(ref):
        ref[...] = jnp.zeros(ref.shape, ref.dtype)

    loads[0].wait()
    for x in range(dx):
        r1[dx + x, 3 : 3 + dy] = jnp.transpose(vol[:, x], (1, 0, 2))

    def packed(raw, j, pair):
        first = jnp.where(lane == j, jnp.broadcast_to(raw[:, 0:1], raw.shape), pair[0])
        last = jnp.where(lane == j, jnp.broadcast_to(raw[:, 127:128], raw.shape), pair[1])
        return first, last

    blank = jnp.zeros((chan, 128), BF16)
    half_lane = lane[0:16]
    edges = [blank[0:16], blank[0:16]]
    for x in range(dx):
        for y in range(dy):
            raw = r1[dx + x, 3 + y]
            for part_of in range(2):
                piece = raw[16 * part_of : 16 * part_of + 16]
                here = half_lane == x * dy + y + 64 * part_of
                for n, column in enumerate((piece[:, 0:1], piece[:, 127:128])):
                    edges[n] = jnp.where(here, jnp.broadcast_to(column, piece.shape), edges[n])
    pk1[0], pk1[1] = edges

    @pl.when(ix == 0)
    def _():
        zero(r1.at[0:dx])
        zero(ed1.at[:, 0])
        zero(r3.at[0])
        zero(ed3.at[:, 0])

    @pl.when(ix == nx - 1)
    def _():
        zero(r1.at[2 * dx : 3 * dx])
        zero(ed1.at[:, 2])
        zero(r3.at[dx + 1])
        zero(ed3.at[:, 2])

    @pl.when(iy == 0)
    def _():
        zero(r1.at[:, 0:3])
        zero(ed1.at[:, :, 0])

    @pl.when(iy == ny - 1)
    def _():
        zero(r1.at[:, 3 + dy : 6 + dy])
        zero(ed1.at[:, :, 2])

    @pl.when(iz == 0)
    def _():
        zero(ed1.at[0])
        zero(ed2.at[0])
        zero(ed3.at[0])

    @pl.when(iz == nz - 1)
    def _():
        zero(ed1.at[1])
        zero(ed2.at[1])
        zero(ed3.at[1])

    def span(index, count):
        return 3 - (index == 0).astype(jnp.int32) - (index == count - 1).astype(jnp.int32)

    near = span(ix, nx) * span(iy, ny) * span(iz, nz) - 1
    pl.semaphore_wait(barrier, near + len(turns) + core * (planes - 1 + len(turns) - 1))

    def send_vol(n):
        (ox, oy, oz), far = VOLUME[n]
        if oz:
            src = pk1.at[1 if oz > 0 else 0]
            dst = ed1.at[0 if oz > 0 else 1, 1 - ox, 1 - oy]
        elif oy == 0:
            own = dx if (ox < 0) != far else 2 * dx - 1
            to = own - dx * ox
            src = r1.at[own, 3 : 3 + dy]
            dst = r1.at[to, 3 : 3 + dy]
        else:
            src_y = 3 if oy < 0 else dy
            dst_y = 0 if oy > 0 else 3 + dy
            to = dx * (1 - ox)
            src = r1.at[dx : 2 * dx, src_y : src_y + 3]
            dst = r1.at[to : to + dx, dst_y : dst_y + 3]
        return copy(src, dst, xs1.at[n], xr1.at[n], at(ox, oy, oz))

    def back(o):
        return there(*(-c for c in o))

    for n, (o, _) in enumerate(VOLUME):
        guarded(there(*o), lambda: send_vol(n).start())

    def take_vol(test):
        for n, (o, far) in enumerate(VOLUME):
            if test(o, far):
                guarded(back(o), lambda: send_vol(n).wait_recv())

    for step in loads[1:]:
        step.wait()
    taps = w_first.shape[0]
    third = taps // 3
    w1t[0:chan, :] = w_first[...].T
    w1t[chan:two, :] = v_first[...].T
    for f, w_ref in enumerate((w_second, v_second)):
        turned = w_ref[...].T
        for kx in range(3):
            w2t[chan * (2 - kx) : chan * (3 - kx), third * f : third * (f + 1)] = turned[:, third * kx : third * (kx + 1)]
    for k in range(27):
        kx, rest = k // 9, k % 9
        w3t[chan * (2 - kx) : chan * (3 - kx), chan * rest : chan * (rest + 1)] = w_second[chan * (26 - k) : chan * (27 - k), :]
    for x in range(dx):
        zero(ej.at[x, 0:3])
        zero(ej.at[x, 3 + dy : 5 + dy])
        zero(eb.at[x, 0:3])
        zero(eb.at[x, 3 + dy : 5 + dy])

    def shift(raw_ref, out_ref, x, y, left, right, j):
        raw = raw_ref[x, y]
        before = left if not j else pltpu.roll(left, 128 - j, 1)
        after = right if j is None else pltpu.roll(right, 127 - j, 1)
        out_ref[x, y, 0:chan] = jnp.where(lane == 0, before, pltpu.roll(raw, 1, 1))
        out_ref[x, y, chan:two] = jnp.where(lane == 127, after, pltpu.roll(raw, 127, 1))

    def turn(raw_ref, out_ref, x, y):
        raw = raw_ref[x, y]
        out_ref[x, y, 0:chan] = pltpu.roll(raw, 1, 1)
        out_ref[x, y, chan:two] = pltpu.roll(raw, 127, 1)

    def patch(out_ref, x, y, left, right, j):
        before = left if not j else pltpu.roll(left, 128 - j, 1)
        after = right if j is None else pltpu.roll(right, 127 - j, 1)
        out_ref[x, y, 0:chan] = jnp.where(lane == 0, before, out_ref[x, y, 0:chan])
        out_ref[x, y, chan:two] = jnp.where(lane == 127, after, out_ref[x, y, chan:two])

    def spread(tile, j, to):
        shifts = [(to - j - 64 * part_of) % 128 for part_of in range(2)]
        return jnp.concatenate([pltpu.roll(tile, k, 1) if k else tile for k in shifts], axis=0)

    def slab1(which, lines, turned=False):
        for x in which:
            for y in lines:
                bx, by = x // dx, (y + dy - 3) // dy
                j = (x % dx) * dy + (y + dy - 3) % dy
                place = (spread(ed1[0, bx, by], j, 0), spread(ed1[1, bx, by], j, 127), None)
                if turned:
                    patch(q1, x, y, *place)
                else:
                    shift(r1, q1, x, y, *place)

    def three(raw_ref, out_ref, x, y):
        return [out_ref[x, y, 0:chan], raw_ref[x, y], out_ref[x, y, chan:two]]

    def layer1(x, y, carry):
        halves = []
        for half in range(2):
            pieces = []
            for kx in range(3):
                for ky in range(3):
                    pieces += three(r1, q1, x + kx, y + half + ky)
            halves.append(jnp.concatenate(pieces, axis=0))
        both = jnp.dot(w1t[...], jnp.concatenate(halves, axis=1), preferred_element_type=F32)
        hidden, slope = gelu_pair(both[0:chan])
        gx_cell = ix * dx + x - 1
        gy_cell = iy * dy + y - 2
        inside = jnp.logical_and(
            jnp.logical_and(gx_cell >= 0, gx_cell < nx * dx), jnp.logical_and(gy_cell >= 0, gy_cell < ny * dy)
        )
        keep = inside.astype(F32)
        tangent = (keep * (slope * both[chan:two])).astype(BF16)
        hidden = (keep * hidden).astype(BF16)
        fields = [carry[0:2], carry[2:4]]
        for half in range(2):
            cols = slice(128 * half, 128 * half + 128)
            for f, value in enumerate((tangent, hidden)):
                r2[f, x, y + half] = value[:, cols]
                fields[f] = packed(value[:, cols], x * hy + y + half, fields[f])
            slope_ref[x, y + half] = slope[:, cols]
        return (*fields[0], *fields[1])

    own_y = range(3, 3 + dy)
    halo_y = [*range(3), *range(3 + dy, 6 + dy)]
    inner = (dy - 4) // 2
    for x in range(dx, 2 * dx):
        for y in own_y:
            turn(r1, q1, x, y)
    take_vol(lambda o, far: o[0] == 0 and o[1] == 0)
    slab1(range(dx, 2 * dx), own_y, True)
    take_vol(lambda o, far: o[0] != 0 and o[1] == 0 and not far)
    slab1((dx - 1, 2 * dx), own_y)
    edges = lax.fori_loop(
        0, dx * inner, lambda i, c: layer1(1 + i // inner, 4 + 2 * lax.rem(i, inner), c), (blank,) * 4, unroll=dx * inner
    )
    take_vol(lambda o, far: o[1] != 0)
    slab1(range(1, 3 * dx - 1), halo_y)

    def outer(i, c):
        k = lax.rem(i, 4)
        return layer1(1 + i // 4, 2 * lax.rem(k, 2) + dy * (k // 2), c)

    edges = lax.fori_loop(0, dx * 4, outer, edges, unroll=8)
    take_vol(lambda o, far: far)
    slab1((0, 3 * dx - 1), range(dy + 6))
    pairs = hy // 2
    edges = lax.fori_loop(
        0, 2 * pairs, lambda i, c: layer1((hx - 1) * (i // pairs), 2 * lax.rem(i, pairs), c), edges, unroll=2 * pairs
    )
    pk2[0, 0], pk2[1, 0], pk2[0, 1], pk2[1, 1] = edges

    def send_hid(n, oz):
        return copy(pk2.at[n], ed2.at[1 - n], xs2.at[n], xr2.at[n], at(0, 0, oz))

    for n, oz in enumerate((-1, 1)):
        guarded(there(0, 0, oz), lambda: send_hid(n, oz).start())
    for f in range(2):
        for x in range(hx):
            for y in range(hy):
                turn(r2.at[f], q2.at[f], x, y)
    for n, oz in enumerate((-1, 1)):
        guarded(there(0, 0, -oz), lambda: send_hid(n, oz).wait_recv())

    for f in range(2):
        for x in range(hx):
            for y in range(hy):
                patch(q2.at[f], x, y, ed2[0, f], ed2[1, f], x * hy + y)

    def layer2(pair, carry):
        y = 2 * pair
        out = [None] * dx
        for x in range(hx):
            halves = []
            for half in range(2):
                pieces = []
                for f in range(2):
                    for ky in range(3):
                        pieces += three(r2.at[f], q2.at[f], x, y + half + ky)
                halves.append(jnp.concatenate(pieces, axis=0))
            low, high = max(0, x - 2), min(dx - 1, x)
            left = w2t[chan * (2 - x + low) : chan * (3 - x + high), :]
            product = jnp.dot(left, jnp.concatenate(halves, axis=1), preferred_element_type=F32)
            for to in range(low, high + 1):
                term = product[chan * (to - low) : chan * (to - low + 1)]
                out[to] = term if out[to] is None else out[to] + term
        for x in range(dx):
            for half in range(2):
                gy_cell = iy * dy + y + half - 1
                keep = jnp.logical_and(gy_cell >= 0, gy_cell < ny * dy).astype(F32)
                value = (keep * out[x][:, 128 * half : 128 * half + 128]).astype(BF16)
                r3[x + 1, y + half] = value
                carry = packed(value, x * (dy + 2) + y + half, carry)
        return carry

    cuts = [0, 8, 14, dy + 2]

    def send_plane(n, ox, late):
        lines = slice(cuts[late], cuts[late + 1])
        return copy(
            r3.at[1 if ox < 0 else dx, lines], r3.at[dx + 1 if ox < 0 else 0, lines],
            ps3.at[n, late], pr3.at[n, late], at(ox, 0, 0),
        )

    def send_jv(n):
        ox, oz = SIDES[n]
        return copy(pk3.at[1 if oz > 0 else 0], ed3.at[0 if oz > 0 else 1, 1 - ox], xs3.at[n], xr3.at[n], at(ox, 0, oz))

    edges = (blank, blank)
    for late in range(3):
        first, count2 = cuts[late] // 2, (cuts[late + 1] - cuts[late]) // 2
        edges = lax.fori_loop(0, count2, lambda i, c: layer2(first + i, c), edges, unroll=count2)
        if late < 2:
            for n, ox in enumerate((-1, 1)):
                guarded(there(ox, 0, 0), lambda: send_plane(n, ox, late).start())
    pk3[0], pk3[1] = edges
    for n, (ox, oz) in enumerate(SIDES):
        guarded(there(ox, 0, oz), lambda: send_jv(n).start())
    for n, ox in enumerate((-1, 1)):
        guarded(there(ox, 0, 0), lambda: send_plane(n, ox, 2).start())

    for x in range(dx):
        own = r3[x + 1, 1 : 1 + dy]
        ej[x, 3 : 3 + dy] = own

    def correlate(raw_ref, out_ref, x0, y0, e_ref):
        total = None
        for x in range(dx):
            lhs, rhs = [], []
            for q in range(dy + 2):
                pieces = []
                for kx in range(3):
                    pieces += three(raw_ref, out_ref, x + kx + x0, q + y0)
                lhs.append(jnp.concatenate(pieces, axis=0))
                rhs.append(jnp.concatenate([e_ref[x, q - ky + 3] for ky in range(4)], axis=0))
            product = lax.dot_general(
                jnp.concatenate(lhs, axis=1), jnp.concatenate(rhs, axis=1),
                (((1,), (1,)), ((), ())), preferred_element_type=F32,
            )
            total = product if total is None else total + product
        return total

    lane8 = lax.broadcasted_iota(jnp.int32, (8, 128), 1)

    def put_part(f, value):
        for t in range(2 * len(turns)):
            if t < 27:
                j, s = t // 9, t % 9
                tail = pltpu.roll(value[216 + 8 * s : 224 + 8 * s], 96 - 32 * j, 1)
                part[t // 2, f, t % 2] = jnp.where(lane8 < 96, value[8 * t : 8 * t + 8], tail)
            else:
                part[t // 2, f, t % 2] = jnp.zeros((8, 128), F32)

    def send_a(f, n):
        eg, ec = turns[n]
        return copy(
            part.at[gs[eg] * wide + cs[ec], f], recv_a.at[f, core * len(turns) + n], sa.at[f], ra.at[f], a_peer(n, 1)
        )

    def send_z(f, d):
        return copy(sum_a.at[f], recv_z.at[f, level], sz.at[f], rz.at[f], z_peer(d))

    def send_g(f, n, side):
        return copy(fin.at[f], tot.at[me, f], sg.at[f], rg.at[f], a_peer(n, side))

    def settle(ref, sem):
        pltpu.make_async_copy(ref, ref, sem).wait()

    count = len(turns)

    def start_a(f, value):
        put_part(f, value)
        for n in range(1, count):
            send_a(f, n).start()

        @pl.when(core == 0)
        def _():
            send_a(f, 0).start()

        @pl.when(core == 1)
        def _():
            recv_a[f, count] = part[me, f]

    def start_z(f):
        @pl.when(core == 1)
        def _():
            settle(recv_a.at[f, 1 : 2 * count], ra.at[f])
            total = recv_a[f, 0]
            for n in range(1, 2 * count):
                total = total + recv_a[f, n]
            sum_a[f] = total
            for d in steps:
                send_z(f, d).start()
            recv_z[f, level] = total

    def start_g(f):
        @pl.when(core == 1)
        def _():
            settle(recv_z.at[f, 1:planes], rz.at[f])
            total = recv_z[f, 0]
            for d in range(1, planes):
                total = total + recv_z[f, d]
            fin[f] = total
            for n in range(1, count):
                send_g(f, n, 0).start()
                send_g(f, n, 1).start()
            send_g(f, 0, 0).start()
            tot[me, f] = total

    def end_g(f):
        @pl.when(core == 1)
        def _():
            settle(recv_a.at[f, 1:count], rg.at[f])

        @pl.when(core == 0)
        def _():
            settle(recv_a.at[f, 0:count], rg.at[f])

    def leave(f):
        @pl.when(core == 1)
        def _():
            settle(recv_a.at[f, 1:count], sa.at[f])
            settle(recv_z.at[f, 1:planes], sz.at[f])
            settle(recv_a.at[f, 1 : 2 * count], sg.at[f])

        @pl.when(core == 0)
        def _():
            settle(recv_a.at[f, 0:count], sa.at[f])

    start_a(0, correlate(r2.at[1], q2.at[1], 0, 1, ej))

    def take_jv(own):
        for n, (ox, oz) in enumerate(SIDES):
            if (ox == 0) == own:
                guarded(there(-ox, 0, -oz), lambda: send_jv(n).wait_recv())

    def slab3(which, turned=False):
        for x in which:
            bx = (x + dx - 1) // dx
            for y in range(dy + 2):
                place = (ed3[0, bx], ed3[1, bx], ((x + dx - 1) % dx) * (dy + 2) + y)
                if turned:
                    patch(q3, x, y, *place)
                else:
                    shift(r3, q3, x, y, *place)

    def layer3(x, y):
        halves = []
        for half in range(2):
            pieces = []
            for ky in range(3):
                pieces += three(r3, q3, x, y + half + ky)
            halves.append(jnp.concatenate(pieces, axis=0))
        low, high = max(0, x - 2), min(dx - 1, x)
        left = w3t[chan * (2 - x + low) : chan * (3 - x + high), :]
        product = jnp.dot(left, jnp.concatenate(halves, axis=1), preferred_element_type=F32)
        return {to: product[chan * (to - low) : chan * (to - low + 1)] for to in range(low, high + 1)}

    for x in range(1, dx + 1):
        for y in range(dy + 2):
            turn(r3, q3, x, y)
    take_jv(True)
    slab3(range(1, dx + 1), True)

    def own3(pair, _):
        y = 2 * pair
        parts = [layer3(x, y) for x in range(1, dx + 1)]
        for x in range(dx):
            summed = parts[0][x] + parts[1][x]
            for half in range(2):
                acc3[x, y + half] = summed[:, 128 * half : 128 * half + 128]
        return 0

    lax.fori_loop(0, dy // 2, own3, 0, unroll=4)
    take_jv(False)
    for n, ox in enumerate((-1, 1)):
        for late in range(3):
            guarded(there(-ox, 0, 0), lambda: send_plane(n, ox, late).wait_recv())
    slab3((0, dx + 1))

    def halo3(pair, _):
        y = 2 * pair
        for x, plane_x in ((0, 0), (dx - 1, dx + 1)):
            term = layer3(plane_x, y)[x]
            for half in range(2):
                cols = slice(128 * half, 128 * half + 128)
                value = slope_ref[x + 1, y + half + 2] * (acc3[x, y + half] + term[:, cols])
                eb[x, y + half + 3] = value.astype(BF16)
        return 0

    lax.fori_loop(0, dy // 2, halo3, 0, unroll=4)

    start_a(1, correlate(r1, q1, 1, 2, eb))
    start_z(0)
    for x in range(dx):
        jv_out[:, x] = jnp.transpose(r3[x + 1, 1 : 1 + dy], (1, 0, 2))
    start_g(0)
    start_z(1)
    start_g(1)
    for f in range(2):
        end_g(f)

    for n, (o, _) in enumerate(VOLUME):
        guarded(there(*o), lambda: send_vol(n).wait_send())
    for n, oz in enumerate((-1, 1)):
        guarded(there(0, 0, oz), lambda: send_hid(n, oz).wait_send())
    for n, ox in enumerate((-1, 1)):
        for late in range(3):
            guarded(there(ox, 0, 0), lambda: send_plane(n, ox, late).wait_send())
    for n, (ox, oz) in enumerate(SIDES):
        guarded(there(ox, 0, oz), lambda: send_jv(n).wait_send())
    for f in range(2):
        leave(f)


def last_kernel(count_all, factor, tot, jv_in, v_first, v_second, jv, gv_first, gv_second):
    jv[...] = jv_in[...]
    for f, (v_ref, out) in enumerate(((v_second, gv_second), (v_first, gv_first))):
        tile = [tot[t // 2, f, t % 2] for t in range(27)]
        for kx in range(3):
            for ky in range(3):
                pieces = []
                for u in range(12 * kx, 12 * kx + 12):
                    if u < 27:
                        piece = tile[u] if ky == 0 else pltpu.roll(tile[u], 128 - 32 * ky, 1)
                    else:
                        piece = pltpu.roll(tile[9 * ky + u - 27], 32, 1)
                    pieces.append(piece[:, 0:32])
                k = 3 * kx + ky
                summed = jnp.concatenate(pieces, axis=0)
                base = v_ref[96 * k : 96 * k + 96, :].astype(F32)
                out[k] = factor * (summed / count_all + 0.1 * base)


def body(volume, w_first, w_second, v_first, v_second):
    chan, dx, dy, dz = volume.shape
    nx, ny, nz = lax.axis_size("gx"), lax.axis_size("gy"), lax.axis_size("gz")
    group = 2 * nz
    planes = nx * ny // 4
    count_all = float(dx * dy * dz * nx * ny * nz)
    factor = math.sqrt(27.0 * chan)
    shape = w_first.shape
    flat = [w.reshape(27 * chan, chan) for w in (w_first, w_second, v_first, v_second)]
    vm = pl.BlockSpec(memory_space=pltpu.VMEM)
    far = functools.partial(pltpu.with_memory_space_constraint, memory_space=pltpu.HBM)
    near = functools.partial(pltpu.with_memory_space_constraint, memory_space=pltpu.VMEM)
    dma = pltpu.SemaphoreType.DMA
    tot, jv_made = pl.pallas_call(
        functools.partial(main_kernel, nx, ny, nz, dx, dy),
        out_shape=(
            pltpu.VMEM((group, 2, 2, 8, 128), F32),
            pltpu.VMEM((chan, dx, dy, 128), BF16),
        ),
        in_specs=[pl.BlockSpec(memory_space=pltpu.HBM)] * 5,
        out_specs=(vm, vm),
        scratch_shapes=[
            pltpu.VMEM(volume.shape, BF16),
            *[pltpu.VMEM(flat[0].shape, BF16)] * 4,
            dma((5,)),
            pltpu.VMEM((3 * dx, dy + 6, chan, 128), BF16),
            pltpu.VMEM((3 * dx, dy + 6, 2 * chan, 128), BF16),
            pltpu.VMEM((2, dx + 2, dy + 4, chan, 128), BF16),
            pltpu.VMEM((2, dx + 2, dy + 4, 2 * chan, 128), BF16),
            pltpu.VMEM((dx + 2, dy + 2, chan, 128), BF16),
            pltpu.VMEM((dx + 2, dy + 2, 2 * chan, 128), BF16),
            pltpu.VMEM((dx + 2, dy + 4, chan, 128), F32),
            pltpu.VMEM((dx, dy, chan, 128), F32),
            pltpu.VMEM((dx, dy + 5, chan, 128), BF16),
            pltpu.VMEM((dx, dy + 5, chan, 128), BF16),
            pltpu.VMEM((2 * chan, 27 * chan), BF16),
            pltpu.VMEM((3 * chan, 18 * chan), BF16),
            pltpu.VMEM((3 * chan, 9 * chan), BF16),
            pltpu.VMEM((2, 16, 128), BF16),
            pltpu.VMEM((2, 3, 3, 16, 128), BF16),
            pltpu.VMEM((2, 2, chan, 128), BF16),
            pltpu.VMEM((2, 2, chan, 128), BF16),
            pltpu.VMEM((2, chan, 128), BF16),
            pltpu.VMEM((2, 3, chan, 128), BF16),
            pltpu.VMEM((group, 2, 2, 8, 128), F32),
            pltpu.VMEM((2, 2 * group, 2, 8, 128), F32),
            pltpu.VMEM((2, 2, 8, 128), F32),
            pltpu.VMEM((2, planes, 2, 8, 128), F32),
            pltpu.VMEM((2, 2, 8, 128), F32),
            dma((len(VOLUME),)), dma((len(VOLUME),)),
            dma((2,)), dma((2,)),
            dma((6,)), dma((6,)),
            dma((2, 3)), dma((2, 3)),
            *[dma((2,))] * 6,
        ],
        compiler_params=pltpu.CompilerParams(collective_id=0, has_side_effects=True, vmem_limit_bytes=40 << 20),
        cost_estimate=pl.CostEstimate(flops=2000000000, bytes_accessed=2000000, transcendentals=400000),
    )(*[far(array) for array in (volume, *flat)])
    jv, gv_first, gv_second = pl.pallas_call(
        functools.partial(last_kernel, count_all, factor),
        out_shape=(
            jax.ShapeDtypeStruct(volume.shape, BF16),
            jax.ShapeDtypeStruct((9, 3 * chan, chan), F32),
            jax.ShapeDtypeStruct((9, 3 * chan, chan), F32),
        ),
        in_specs=[vm] * 4,
        out_specs=(vm, vm, vm),
        compiler_params=pltpu.CompilerParams(vmem_limit_bytes=8 << 20),
    )(near(tot), near(jv_made), flat[2], flat[3])
    return (jv, gv_first.reshape(shape), gv_second.reshape(shape))


def solution(mesh):
    in_specs = (P(None, "gx", "gy", "gz"), P(), P(), P(), P())
    out_specs = (P(None, "gx", "gy", "gz"), P(), P())
    return jax.shard_map(body, mesh=mesh, in_specs=in_specs, out_specs=out_specs, check_vma=False)
```

```python
import functools
import itertools
import math

import jax
import jax.numpy as jnp
from jax import lax
from jax.experimental import pallas as pl
from jax.experimental.pallas import tpu as pltpu
from jax.sharding import PartitionSpec as P

MESH = pl.DeviceIdType.MESH
BF16 = jnp.bfloat16
F32 = jnp.float32
OFFSETS = [o for o in itertools.product((-1, 0, 1), repeat=3) if o != (0, 0, 0)]
VOLUME = []
VOLUME += [(o, False) for o in OFFSETS if o[1] != 0 and o[2] != 0]
VOLUME += [(o, False) for o in OFFSETS if o[1] != 0 and o[0] == 0 and o[2] == 0]
VOLUME += [(o, False) for o in OFFSETS if o[1] != 0 and o[0] != 0 and o[2] == 0]
VOLUME += [((ox, 0, oz), False) for ox in (0, -1, 1) for oz in (-1, 1)]
VOLUME += [((ox, 0, 0), False) for ox in (-1, 1)]
VOLUME += [((ox, 0, 0), True) for ox in (-1, 1)]
SIDES = [(ox, oz) for ox in (-1, 0, 1) for oz in (-1, 1)]


def gelu_pair(pre):
    square = pre * pre
    hyper = jnp.tanh(0.7978845608 * (pre + 0.044715 * square * pre))
    half = 0.5 * (1.0 + hyper)
    hidden = pre * half
    slope = half + (0.5 * pre) * (1.0 - hyper * hyper) * (0.7978845608 * (1.0 + 0.134145 * square))
    return (hidden, slope)


def main_kernel(
    nx, ny, nz, dx, dy,
    vol_in, w_first_in, w_second_in, v_first_in, v_second_in,
    tot, jv_out,
    vol, w_first, w_second, v_first, v_second, load, r1, q1, r2, q2, r3, q3, slope_ref, acc3, ej, eb, w1t, w2t, w3t,
    pk1, ed1, pk2, ed2, pk3, ed3,
    part, recv_a, sum_a, recv_z, fin,
    xs1, xr1, xs2, xr2, xs3, xr3, ps3, pr3,
    sa, ra, sz, rz, sg, rg,
):
    ix, iy, iz = lax.axis_index("gx"), lax.axis_index("gy"), lax.axis_index("gz")
    me = iy * nx + ix
    chan = vol.shape[0]
    two = 2 * chan
    hx, hy = dx + 2, dy + 4
    lane = lax.broadcasted_iota(jnp.int32, (chan, 128), 1)

    def there(ox, oy, oz):
        ok = None
        for offset, index, count in ((ox, ix, nx), (oy, iy, ny), (oz, iz, nz)):
            if offset:
                one = index < count - 1 if offset > 0 else index > 0
                ok = one if ok is None else jnp.logical_and(ok, one)
        return ok

    def at(ox, oy, oz):
        return {"gx": ix + ox, "gy": iy + oy, "gz": iz + oz}

    wide = 4
    high = ny // wide
    planes = high * nx
    col, row = lax.rem(iy, wide), iy // wide
    level = row * nx + ix
    rings = nz // 2
    core, ring = lax.rem(iz, 2), iz // 2
    gs = [lax.rem(ring + d, rings) for d in range(rings)]
    cs = [lax.rem(col + d, wide) for d in range(wide)]
    turns = sorted(
        ((eg, ec) for eg in range(rings) for ec in range(wide)),
        key=lambda t: (t != (0, 0), -min(t[0], rings - t[0]) - min(t[1], wide - t[1])),
    )
    steps = sorted(range(1, planes), key=lambda d: -min(d, planes - d))
    me = ring * wide + col

    def a_peer(n, side):
        eg, ec = turns[n]
        return {"gx": ix, "gy": row * wide + cs[ec], "gz": 2 * gs[eg] + side}

    def z_peer(d):
        other = lax.rem(level + d, planes)
        return {"gx": lax.rem(other, nx), "gy": (other // nx) * wide + col, "gz": iz}

    def copy(src, dst, send, recv, peer):
        return pltpu.make_async_remote_copy(src, dst, send, recv, device_id=peer, device_id_type=MESH)

    def guarded(cond, action):
        @pl.when(cond)
        def _():
            action()

    loads = [
        pltpu.make_async_copy(src, dst, load.at[n])
        for n, (src, dst) in enumerate(
            ((vol_in, vol), (w_first_in, w_first), (w_second_in, w_second), (v_first_in, v_first), (v_second_in, v_second))
        )
    ]
    for step in loads:
        step.start()
    barrier = pltpu.get_barrier_semaphore()

    def greet(peer):
        pl.semaphore_signal(barrier, inc=1, device_id=peer, device_id_type=MESH)

    @pl.when(core == 1)
    def _():
        for d in range(1, planes):
            greet(z_peer(d))
        for n in range(1, len(turns)):
            greet(a_peer(n, 0))

    for n in range(1, len(turns)):
        greet(a_peer(n, 1))
    greet(a_peer(0, 1 - core))
    for o in OFFSETS:
        guarded(there(*o), lambda: greet(at(*o)))

    def zero(ref):
        ref[...] = jnp.zeros(ref.shape, ref.dtype)

    loads[0].wait()
    for x in range(dx):
        r1[dx + x, 3 : 3 + dy] = jnp.transpose(vol[:, x], (1, 0, 2))

    def packed(raw, j, pair):
        first = jnp.where(lane == j, jnp.broadcast_to(raw[:, 0:1], raw.shape), pair[0])
        last = jnp.where(lane == j, jnp.broadcast_to(raw[:, 127:128], raw.shape), pair[1])
        return first, last

    blank = jnp.zeros((chan, 128), BF16)
    half_lane = lane[0:8]
    edges = [blank[0:8], blank[0:8]]
    for x in range(dx):
        for y in range(dy):
            raw = r1[dx + x, 3 + y]
            for part_of in range(4):
                piece = raw[8 * part_of : 8 * part_of + 8]
                here = half_lane == x * dy + y + 32 * part_of
                for n, column in enumerate((piece[:, 0:1], piece[:, 127:128])):
                    edges[n] = jnp.where(here, jnp.broadcast_to(column, piece.shape), edges[n])
    pk1[0], pk1[1] = edges

    @pl.when(ix == 0)
    def _():
        zero(r1.at[dx - 1])
        zero(r2.at[:, 0])
        zero(ed1.at[:, 0])
        zero(r3.at[0])
        zero(ed3.at[:, 0])

    @pl.when(ix == nx - 1)
    def _():
        zero(r1.at[2 * dx])
        zero(r2.at[:, hx - 1])
        zero(ed1.at[:, 2])
        zero(r3.at[dx + 1])
        zero(ed3.at[:, 2])

    @pl.when(iy == 0)
    def _():
        zero(r1.at[:, 0:3])
        zero(ed1.at[:, :, 0])

    @pl.when(iy == ny - 1)
    def _():
        zero(r1.at[:, 3 + dy : 6 + dy])
        zero(ed1.at[:, :, 2])

    @pl.when(iz == 0)
    def _():
        zero(ed1.at[0])
        zero(ed2.at[0])
        zero(ed3.at[0])

    @pl.when(iz == nz - 1)
    def _():
        zero(ed1.at[1])
        zero(ed2.at[1])
        zero(ed3.at[1])

    def span(index, count):
        return 3 - (index == 0).astype(jnp.int32) - (index == count - 1).astype(jnp.int32)

    near = span(ix, nx) * span(iy, ny) * span(iz, nz) - 1
    pl.semaphore_wait(barrier, near + len(turns) + core * (planes - 1 + len(turns) - 1))

    def send_vol(n):
        (ox, oy, oz), far = VOLUME[n]
        if oz:
            src = pk1.at[1 if oz > 0 else 0]
            dst = ed1.at[0 if oz > 0 else 1, 1 - ox, 1 - oy]
        elif oy == 0:
            own = dx if (ox < 0) != far else 2 * dx - 1
            to = own - dx * ox
            src = r1.at[own, 3 : 3 + dy]
            dst = r1.at[to, 3 : 3 + dy]
        else:
            src_y = 3 if oy < 0 else dy
            dst_y = 0 if oy > 0 else 3 + dy
            to = dx * (1 - ox)
            src = r1.at[dx : 2 * dx, src_y : src_y + 3]
            dst = r1.at[to : to + dx, dst_y : dst_y + 3]
        return copy(src, dst, xs1.at[0], xr1.at[n], at(ox, oy, oz))

    def back(o):
        return there(*(-c for c in o))

    for n, (o, _) in enumerate(VOLUME):
        guarded(there(*o), lambda: send_vol(n).start())

    def take_vol(test):
        for n, (o, far) in enumerate(VOLUME):
            if test(o, far):
                guarded(back(o), lambda: send_vol(n).wait_recv())

    for step in loads[1:]:
        step.wait()
    taps = w_first.shape[0]
    third = taps // 3
    w1t[0:chan, :] = w_first[...].T
    w1t[chan:two, :] = v_first[...].T
    for f, w_ref in enumerate((w_second, v_second)):
        turned = w_ref[...].T
        for kx in range(3):
            w2t[chan * (2 - kx) : chan * (3 - kx), third * f : third * (f + 1)] = turned[:, third * kx : third * (kx + 1)]
    for k in range(27):
        kx, rest = k // 9, k % 9
        w3t[chan * (2 - kx) : chan * (3 - kx), chan * rest : chan * (rest + 1)] = w_second[chan * (26 - k) : chan * (27 - k), :]
    for x in range(dx):
        zero(ej.at[x, 0:3])
        zero(ej.at[x, 3 + dy : 5 + dy])
        zero(eb.at[x, 0:3])
        zero(eb.at[x, 3 + dy : 5 + dy])

    def shift(raw_ref, out_ref, x, y, left, right, j):
        raw = raw_ref[x, y]
        before = left if not j else pltpu.roll(left, 128 - j, 1)
        after = right if j is None else pltpu.roll(right, 127 - j, 1)
        out_ref[x, y, 0:chan] = jnp.where(lane == 0, before, pltpu.roll(raw, 1, 1))
        out_ref[x, y, chan:two] = jnp.where(lane == 127, after, pltpu.roll(raw, 127, 1))

    def turn(raw_ref, out_ref, x, y):
        raw = raw_ref[x, y]
        out_ref[x, y, 0:chan] = pltpu.roll(raw, 1, 1)
        out_ref[x, y, chan:two] = pltpu.roll(raw, 127, 1)

    def patch(out_ref, x, y, left, right, j):
        before = left if not j else pltpu.roll(left, 128 - j, 1)
        after = right if j is None else pltpu.roll(right, 127 - j, 1)
        out_ref[x, y, 0:chan] = jnp.where(lane == 0, before, out_ref[x, y, 0:chan])
        out_ref[x, y, chan:two] = jnp.where(lane == 127, after, out_ref[x, y, chan:two])

    def spread(tile, j, to):
        shifts = [(to - j - 32 * part_of) % 128 for part_of in range(4)]
        return jnp.concatenate([pltpu.roll(tile, k, 1) if k else tile for k in shifts], axis=0)

    def slab1(which, lines, turned=False):
        for x in which:
            for y in lines:
                bx, by = x // dx, (y + dy - 3) // dy
                j = (x % dx) * dy + (y + dy - 3) % dy
                place = (spread(ed1[0, bx, by], j, 0), spread(ed1[1, bx, by], j, 127), None)
                if turned:
                    patch(q1, x, y, *place)
                else:
                    shift(r1, q1, x, y, *place)

    def three(raw_ref, out_ref, x, y):
        return [out_ref[x, y, 0:chan], raw_ref[x, y], out_ref[x, y, chan:two]]

    def layer1(x, y, carry):
        halves = []
        for half in range(2):
            pieces = []
            for kx in range(3):
                for ky in range(3):
                    pieces += three(r1, q1, x + kx, y + half + ky)
            halves.append(jnp.concatenate(pieces, axis=0))
        both = jnp.dot(w1t[...], jnp.concatenate(halves, axis=1), preferred_element_type=F32)
        hidden, slope = gelu_pair(both[0:chan])
        gx_cell = ix * dx + x - 1
        gy_cell = iy * dy + y - 2
        inside = jnp.logical_and(
            jnp.logical_and(gx_cell >= 0, gx_cell < nx * dx), jnp.logical_and(gy_cell >= 0, gy_cell < ny * dy)
        )
        keep = inside.astype(F32)
        tangent = (keep * (slope * both[chan:two])).astype(BF16)
        hidden = (keep * hidden).astype(BF16)
        fields = [carry[0:2], carry[2:4]]
        for half in range(2):
            cols = slice(128 * half, 128 * half + 128)
            for f, value in enumerate((tangent, hidden)):
                r2[f, x, y + half] = value[:, cols]
                fields[f] = packed(value[:, cols], x * hy + y + half, fields[f])
            slope_ref[x, y + half] = slope[:, cols]
        return (*fields[0], *fields[1])

    own_y = range(3, 3 + dy)
    halo_y = [*range(3), *range(3 + dy, 6 + dy)]
    pairs = hy // 2

    def line1(x, carry):
        return lax.fori_loop(0, pairs, lambda i, c: layer1(x, 2 * i, c), carry, unroll=pairs)

    def low_near():
        take_vol(lambda o, far: o == (1, 0, 0) and not far)
        slab1((dx - 1,), own_y)

    def high_near():
        take_vol(lambda o, far: o == (-1, 0, 0) and not far)
        slab1((2 * dx,), own_y)

    low_first = ix == 0
    first = jnp.where(low_first, 1, 2)
    for x in range(dx, 2 * dx):
        for y in own_y:
            turn(r1, q1, x, y)
    take_vol(lambda o, far: o[1] == 0 and o[2] != 0)
    slab1(range(dx, 2 * dx), own_y, True)
    guarded(low_first, low_near)
    guarded(jnp.logical_not(low_first), high_near)
    take_vol(lambda o, far: o[1] != 0)
    slab1(range(1, 3 * dx - 1), halo_y)
    edges = line1(first, (blank,) * 4)
    guarded(low_first, high_near)
    guarded(jnp.logical_not(low_first), low_near)
    edges = line1(3 - first, edges)

    def low_end(carry):
        take_vol(lambda o, far: far and o[0] > 0)
        slab1((0,), range(dy + 6))
        return line1(0, carry)

    def high_end(carry):
        take_vol(lambda o, far: far and o[0] < 0)
        slab1((3 * dx - 1,), range(dy + 6))
        return line1(hx - 1, carry)

    edges = lax.cond(there(-1, 0, 0), low_end, lambda c: c, edges)
    edges = lax.cond(there(1, 0, 0), high_end, lambda c: c, edges)
    pk2[0, 0], pk2[1, 0], pk2[0, 1], pk2[1, 1] = edges

    def send_hid(n, oz):
        return copy(pk2.at[n], ed2.at[1 - n], xs2.at[n], xr2.at[n], at(0, 0, oz))

    for n, oz in enumerate((-1, 1)):
        guarded(there(0, 0, oz), lambda: send_hid(n, oz).start())
    for f in range(2):
        for x in range(hx):
            for y in range(hy):
                turn(r2.at[f], q2.at[f], x, y)
    for n, oz in enumerate((-1, 1)):
        guarded(there(0, 0, -oz), lambda: send_hid(n, oz).wait_recv())

    for f in range(2):
        for x in range(hx):
            for y in range(hy):
                patch(q2.at[f], x, y, ed2[0, f], ed2[1, f], x * hy + y)

    def layer2(pair, carry):
        y = 2 * pair
        out = [None] * dx
        for x in range(hx):
            halves = []
            for half in range(2):
                pieces = []
                for f in range(2):
                    for ky in range(3):
                        pieces += three(r2.at[f], q2.at[f], x, y + half + ky)
                halves.append(jnp.concatenate(pieces, axis=0))
            low, high = max(0, x - 2), min(dx - 1, x)
            left = w2t[chan * (2 - x + low) : chan * (3 - x + high), :]
            product = jnp.dot(left, jnp.concatenate(halves, axis=1), preferred_element_type=F32)
            for to in range(low, high + 1):
                term = product[chan * (to - low) : chan * (to - low + 1)]
                out[to] = term if out[to] is None else out[to] + term
        for x in range(dx):
            for half in range(2):
                gy_cell = iy * dy + y + half - 1
                keep = jnp.logical_and(gy_cell >= 0, gy_cell < ny * dy).astype(F32)
                value = (keep * out[x][:, 128 * half : 128 * half + 128]).astype(BF16)
                r3[x + 1, y + half] = value
                carry = packed(value, x * (dy + 2) + y + half, carry)
        return carry

    cuts = [0, 8, 14, dy + 2]

    def send_plane(n, ox, late):
        lines = slice(cuts[late], cuts[late + 1])
        return copy(
            r3.at[1 if ox < 0 else dx, lines], r3.at[dx + 1 if ox < 0 else 0, lines],
            ps3.at[n, late], pr3.at[n, late], at(ox, 0, 0),
        )

    def send_jv(n):
        ox, oz = SIDES[n]
        return copy(pk3.at[1 if oz > 0 else 0], ed3.at[0 if oz > 0 else 1, 1 - ox], xs3.at[n], xr3.at[n], at(ox, 0, oz))

    edges = (blank, blank)
    for late in range(3):
        first, count2 = cuts[late] // 2, (cuts[late + 1] - cuts[late]) // 2
        edges = lax.fori_loop(0, count2, lambda i, c: layer2(first + i, c), edges, unroll=count2)
        if late < 2:
            for n, ox in enumerate((-1, 1)):
                guarded(there(ox, 0, 0), lambda: send_plane(n, ox, late).start())
    pk3[0], pk3[1] = edges
    for n, (ox, oz) in enumerate(SIDES):
        guarded(there(ox, 0, oz), lambda: send_jv(n).start())
    for n, ox in enumerate((-1, 1)):
        guarded(there(ox, 0, 0), lambda: send_plane(n, ox, 2).start())

    for x in range(dx):
        own = r3[x + 1, 1 : 1 + dy]
        ej[x, 3 : 3 + dy] = own

    def correlate(raw_ref, out_ref, x0, y0, e_ref):
        total = None
        for x in range(dx):
            lhs, rhs = [], []
            for q in range(dy + 2):
                pieces = []
                for kx in range(3):
                    pieces += three(raw_ref, out_ref, x + kx + x0, q + y0)
                lhs.append(jnp.concatenate(pieces, axis=0))
                rhs.append(jnp.concatenate([e_ref[x, q - ky + 3] for ky in range(4)], axis=0))
            product = lax.dot_general(
                jnp.concatenate(lhs, axis=1), jnp.concatenate(rhs, axis=1),
                (((1,), (1,)), ((), ())), preferred_element_type=F32,
            )
            total = product if total is None else total + product
        return total

    lane8 = lax.broadcasted_iota(jnp.int32, (8, 128), 1)

    def put_part(f, value):
        for t in range(2 * len(turns)):
            if t < 27:
                j, s = t // 9, t % 9
                tail = pltpu.roll(value[216 + 8 * s : 224 + 8 * s], 96 - 32 * j, 1)
                part[t // 2, f, t % 2] = jnp.where(lane8 < 96, value[8 * t : 8 * t + 8], tail)
            else:
                part[t // 2, f, t % 2] = jnp.zeros((8, 128), F32)

    def send_a(f, n):
        eg, ec = turns[n]
        return copy(
            part.at[gs[eg] * wide + cs[ec], f], recv_a.at[f, core * len(turns) + n], sa.at[f], ra.at[f], a_peer(n, 1)
        )

    def send_z(f, d):
        return copy(sum_a.at[f], recv_z.at[f, level], sz.at[f], rz.at[f], z_peer(d))

    def send_g(f, n, side):
        return copy(fin.at[f], tot.at[me, f], sg.at[f], rg.at[f], a_peer(n, side))

    def settle(ref, sem):
        pltpu.make_async_copy(ref, ref, sem).wait()

    count = len(turns)

    def start_a(f, value):
        put_part(f, value)
        for n in range(1, count):
            send_a(f, n).start()

        @pl.when(core == 0)
        def _():
            send_a(f, 0).start()

        @pl.when(core == 1)
        def _():
            recv_a[f, count] = part[me, f]

    def start_z(f):
        @pl.when(core == 1)
        def _():
            settle(recv_a.at[f, 1 : 2 * count], ra.at[f])
            total = recv_a[f, 0]
            for n in range(1, 2 * count):
                total = total + recv_a[f, n]
            sum_a[f] = total
            for d in steps:
                send_z(f, d).start()
            recv_z[f, level] = total

    def start_g(f):
        @pl.when(core == 1)
        def _():
            settle(recv_z.at[f, 1:planes], rz.at[f])
            total = recv_z[f, 0]
            for d in range(1, planes):
                total = total + recv_z[f, d]
            fin[f] = total
            for n in range(1, count):
                send_g(f, n, 0).start()
                send_g(f, n, 1).start()
            send_g(f, 0, 0).start()
            tot[me, f] = total

    def end_g(f):
        @pl.when(core == 1)
        def _():
            settle(recv_a.at[f, 1:count], rg.at[f])

        @pl.when(core == 0)
        def _():
            settle(recv_a.at[f, 0:count], rg.at[f])

    def leave(f):
        @pl.when(core == 1)
        def _():
            settle(recv_a.at[f, 1:count], sa.at[f])
            settle(recv_z.at[f, 1:planes], sz.at[f])
            settle(recv_a.at[f, 1 : 2 * count], sg.at[f])

        @pl.when(core == 0)
        def _():
            settle(recv_a.at[f, 0:count], sa.at[f])

    start_a(0, correlate(r2.at[1], q2.at[1], 0, 1, ej))

    def take_jv(own):
        for n, (ox, oz) in enumerate(SIDES):
            if (ox == 0) == own:
                guarded(there(-ox, 0, -oz), lambda: send_jv(n).wait_recv())

    def slab3(which, turned=False):
        for x in which:
            bx = (x + dx - 1) // dx
            for y in range(dy + 2):
                place = (ed3[0, bx], ed3[1, bx], ((x + dx - 1) % dx) * (dy + 2) + y)
                if turned:
                    patch(q3, x, y, *place)
                else:
                    shift(r3, q3, x, y, *place)

    def layer3(x, y):
        halves = []
        for half in range(2):
            pieces = []
            for ky in range(3):
                pieces += three(r3, q3, x, y + half + ky)
            halves.append(jnp.concatenate(pieces, axis=0))
        low, high = max(0, x - 2), min(dx - 1, x)
        left = w3t[chan * (2 - x + low) : chan * (3 - x + high), :]
        product = jnp.dot(left, jnp.concatenate(halves, axis=1), preferred_element_type=F32)
        return {to: product[chan * (to - low) : chan * (to - low + 1)] for to in range(low, high + 1)}

    for x in range(1, dx + 1):
        for y in range(dy + 2):
            turn(r3, q3, x, y)
    take_jv(True)
    slab3(range(1, dx + 1), True)

    def own3(pair, _):
        y = 2 * pair
        parts = [layer3(x, y) for x in range(1, dx + 1)]
        for x in range(dx):
            summed = parts[0][x] + parts[1][x]
            for half in range(2):
                acc3[x, y + half] = summed[:, 128 * half : 128 * half + 128]
        return 0

    lax.fori_loop(0, dy // 2, own3, 0, unroll=4)
    take_jv(False)
    for n, ox in enumerate((-1, 1)):
        for late in range(3):
            guarded(there(-ox, 0, 0), lambda: send_plane(n, ox, late).wait_recv())
    slab3((0, dx + 1))

    def halo3(pair, _):
        y = 2 * pair
        for x, plane_x in ((0, 0), (dx - 1, dx + 1)):
            term = layer3(plane_x, y)[x]
            for half in range(2):
                cols = slice(128 * half, 128 * half + 128)
                value = slope_ref[x + 1, y + half + 2] * (acc3[x, y + half] + term[:, cols])
                eb[x, y + half + 3] = value.astype(BF16)
        return 0

    lax.fori_loop(0, dy // 2, halo3, 0, unroll=4)

    start_a(1, correlate(r1, q1, 1, 2, eb))
    start_z(0)
    for x in range(dx):
        jv_out[:, x] = jnp.transpose(r3[x + 1, 1 : 1 + dy], (1, 0, 2))
    start_g(0)
    start_z(1)
    start_g(1)
    for f in range(2):
        end_g(f)

    for n, (o, _) in enumerate(VOLUME):
        guarded(there(*o), lambda: send_vol(n).wait_send())
    for n, oz in enumerate((-1, 1)):
        guarded(there(0, 0, oz), lambda: send_hid(n, oz).wait_send())
    for n, ox in enumerate((-1, 1)):
        for late in range(3):
            guarded(there(ox, 0, 0), lambda: send_plane(n, ox, late).wait_send())
    for n, (ox, oz) in enumerate(SIDES):
        guarded(there(ox, 0, oz), lambda: send_jv(n).wait_send())
    for f in range(2):
        leave(f)


def last_kernel(count_all, factor, tot, jv_in, v_first, v_second, jv, gv_first, gv_second):
    jv[...] = jv_in[...]
    for f, (v_ref, out) in enumerate(((v_second, gv_second), (v_first, gv_first))):
        tile = [tot[t // 2, f, t % 2] for t in range(27)]
        for kx in range(3):
            for ky in range(3):
                pieces = []
                for u in range(12 * kx, 12 * kx + 12):
                    if u < 27:
                        piece = tile[u] if ky == 0 else pltpu.roll(tile[u], 128 - 32 * ky, 1)
                    else:
                        piece = pltpu.roll(tile[9 * ky + u - 27], 32, 1)
                    pieces.append(piece[:, 0:32])
                k = 3 * kx + ky
                summed = jnp.concatenate(pieces, axis=0)
                base = v_ref[96 * k : 96 * k + 96, :].astype(F32)
                out[k] = factor * (summed / count_all + 0.1 * base)


def body(volume, w_first, w_second, v_first, v_second):
    chan, dx, dy, dz = volume.shape
    nx, ny, nz = lax.axis_size("gx"), lax.axis_size("gy"), lax.axis_size("gz")
    group = 2 * nz
    planes = nx * ny // 4
    count_all = float(dx * dy * dz * nx * ny * nz)
    factor = math.sqrt(27.0 * chan)
    shape = w_first.shape
    flat = [w.reshape(27 * chan, chan) for w in (w_first, w_second, v_first, v_second)]
    vm = pl.BlockSpec(memory_space=pltpu.VMEM)
    far = functools.partial(pltpu.with_memory_space_constraint, memory_space=pltpu.HBM)
    near = functools.partial(pltpu.with_memory_space_constraint, memory_space=pltpu.VMEM)
    dma = pltpu.SemaphoreType.DMA
    tot, jv_made = pl.pallas_call(
        functools.partial(main_kernel, nx, ny, nz, dx, dy),
        out_shape=(
            pltpu.VMEM((group, 2, 2, 8, 128), F32),
            pltpu.VMEM((chan, dx, dy, 128), BF16),
        ),
        in_specs=[pl.BlockSpec(memory_space=pltpu.HBM)] * 5,
        out_specs=(vm, vm),
        scratch_shapes=[
            pltpu.VMEM(volume.shape, BF16),
            *[pltpu.VMEM(flat[0].shape, BF16)] * 4,
            dma((5,)),
            pltpu.VMEM((3 * dx, dy + 6, chan, 128), BF16),
            pltpu.VMEM((3 * dx, dy + 6, 2 * chan, 128), BF16),
            pltpu.VMEM((2, dx + 2, dy + 4, chan, 128), BF16),
            pltpu.VMEM((2, dx + 2, dy + 4, 2 * chan, 128), BF16),
            pltpu.VMEM((dx + 2, dy + 2, chan, 128), BF16),
            pltpu.VMEM((dx + 2, dy + 2, 2 * chan, 128), BF16),
            pltpu.VMEM((dx + 2, dy + 4, chan, 128), F32),
            pltpu.VMEM((dx, dy, chan, 128), F32),
            pltpu.VMEM((dx, dy + 5, chan, 128), BF16),
            pltpu.VMEM((dx, dy + 5, chan, 128), BF16),
            pltpu.VMEM((2 * chan, 27 * chan), BF16),
            pltpu.VMEM((3 * chan, 18 * chan), BF16),
            pltpu.VMEM((3 * chan, 9 * chan), BF16),
            pltpu.VMEM((2, 8, 128), BF16),
            pltpu.VMEM((2, 3, 3, 8, 128), BF16),
            pltpu.VMEM((2, 2, chan, 128), BF16),
            pltpu.VMEM((2, 2, chan, 128), BF16),
            pltpu.VMEM((2, chan, 128), BF16),
            pltpu.VMEM((2, 3, chan, 128), BF16),
            pltpu.VMEM((group, 2, 2, 8, 128), F32),
            pltpu.VMEM((2, 2 * group, 2, 8, 128), F32),
            pltpu.VMEM((2, 2, 8, 128), F32),
            pltpu.VMEM((2, planes, 2, 8, 128), F32),
            pltpu.VMEM((2, 2, 8, 128), F32),
            dma((1,)), dma((len(VOLUME),)),
            dma((2,)), dma((2,)),
            dma((6,)), dma((6,)),
            dma((2, 3)), dma((2, 3)),
            *[dma((2,))] * 6,
        ],
        compiler_params=pltpu.CompilerParams(collective_id=0, has_side_effects=True, vmem_limit_bytes=40 << 20),
        cost_estimate=pl.CostEstimate(flops=2000000000, bytes_accessed=2000000, transcendentals=400000),
    )(*[far(array) for array in (volume, *flat)])
    jv, gv_first, gv_second = pl.pallas_call(
        functools.partial(last_kernel, count_all, factor),
        out_shape=(
            jax.ShapeDtypeStruct(volume.shape, BF16),
            jax.ShapeDtypeStruct((9, 3 * chan, chan), F32),
            jax.ShapeDtypeStruct((9, 3 * chan, chan), F32),
        ),
        in_specs=[vm] * 4,
        out_specs=(vm, vm, vm),
        compiler_params=pltpu.CompilerParams(vmem_limit_bytes=8 << 20),
    )(near(tot), near(jv_made), flat[2], flat[3])
    return (jv, gv_first.reshape(shape), gv_second.reshape(shape))


def solution(mesh):
    in_specs = (P(None, "gx", "gy", "gz"), P(), P(), P(), P())
    out_specs = (P(None, "gx", "gy", "gz"), P(), P())
    return jax.shard_map(body, mesh=mesh, in_specs=in_specs, out_specs=out_specs, check_vma=False)
```
